256 devices in a mesh: rep: 4 (over x), fsdp: 32 (over y, z), tp: 2 (over core).
Axes of the slice: x: 4, y: 4, z: 8, core: 2. Of those that a mesh axis runs over, the one named last changes fastest.
Arguments:
- saved_inputs: bfloat16 [2, 32768, 768], P(None, ('rep', 'fsdp')), may hold values from -24 to 24
- out_cotangent: float32 [32768, 768], P(('rep', 'fsdp')), may hold values from -1.75 to 1.75
- gate_weight: bfloat16 [2, 768, 4480], P(None, 'fsdp', 'tp'), may hold values from -0.21875 to 0.21875
- up_weight: bfloat16 [2, 768, 4480], P(None, 'fsdp', 'tp'), may hold values from -0.21875 to 0.21875
- down_weight: bfloat16 [2, 768, 4480], P(None, 'fsdp', 'tp'), may hold values from -0.09375 to 0.09375
- norm_gain: bfloat16 [2, 768], P(None, 'fsdp'), may hold values from 0.5 to 1.5
- gate_accum: float32 [2, 768, 4480], P(None, 'fsdp', 'tp'), may hold values from -12 to 12
- up_accum: float32 [2, 768, 4480], P(None, 'fsdp', 'tp'), may hold values from -12 to 12
- down_accum: float32 [2, 768, 4480], P(None, 'fsdp', 'tp'), may hold values from -12 to 12
- gain_accum: float32 [2, 768], P(None, 'fsdp'), may hold values from -12 to 12
Outputs:
- input_cotangent: float32 [32768, 768], P(('rep', 'fsdp'))
- gate_grad: float32 [2, 768, 4480], P(None, 'fsdp', 'tp')
- up_grad: float32 [2, 768, 4480], P(None, 'fsdp', 'tp')
- down_grad: float32 [2, 768, 4480], P(None, 'fsdp', 'tp')
- gain_grad: float32 [2, 768], P(None, 'fsdp')
The draws below stay inside these ranges and needn't reach their ends.
All inputs are finite; a program needn't handle non-finite values.
Results may differ from the reference program's by a relative error of at most 0.0025.
Values may be sent and summed in bfloat16 or wider, within the bound.
No kernel may reach another device: no remote copies, remote signals or barrier semaphores. Data moves between devices by JAX's collectives and lax.ppermute only.
A program may use at most 192 MiB of HBM per device.

```python
import jax
import jax.numpy as jnp
from jax import lax

LAYERS = 2
D = 768
FF = 4480
TOK_DEV = 256
TOKENS = 32768
N_REP = 4
N_FSDP = 32


def with_spikes(array, stream_key, source, target, parts, factor):
    def block_of(position):
        return (jnp.arange(array.shape[position]) // (array.shape[position] // parts)).reshape((-1,) + (1,) * (array.ndim - 1 - position))

    near = jax.random.permutation(stream_key, parts)[block_of(target)]
    second = (block_of(target) + parts // 2) % parts
    return jnp.where((block_of(source) == near) | (block_of(source) == second), factor * array, array)


def block_levels(rng, shape, shards, smallest, top_value):
    gain, own = 1.0, jax.random.fold_in(rng, 6)
    for dim, parts in shards:
        steps = jnp.exp(jax.random.uniform(jax.random.fold_in(own, dim), (parts,), jnp.float32, smallest / len(shards), top_value / len(shards)))
        gain = gain * jnp.repeat(steps, shape[dim] // parts).reshape([-1 if axis == dim else 1 for axis in range(len(shape))])
    return gain


def normal_values(rng, shape, deviation, most, shards=(), dtype=jnp.bfloat16):
    gain = block_levels(rng, shape, shards, -0.22, 0.18) if shards else 1.0
    values = jax.random.normal(rng, shape, jnp.float32) * deviation * gain
    return jnp.minimum(jnp.maximum(values, -most), most).astype(dtype)


def bell_draw_with(own_key, dims, width, limit, pieces, heavy, dtype=jnp.bfloat16):
    values = width * jax.random.normal(own_key, dims, jnp.float32)
    if pieces:
        values = values * block_levels(own_key, dims, pieces, -0.22, 0.18)
    return jnp.clip(with_spikes(values, jax.random.fold_in(own_key, 3), *heavy), -limit, limit).astype(dtype)


def setup_inputs(seed: int = 0) -> dict:
    keys = jax.random.split(jax.random.key(seed), 11)
    return {
        "saved_inputs": bell_draw_with(keys[0], (LAYERS, TOKENS, D), 1.0, 24.0, ((1, 128),), (1, 2, 128, 5.5)),
        "out_cotangent": bell_draw_with(keys[1], (TOKENS, D), (TOKENS ** -0.25), 1.75, ((0, 128),), (0, 1, 128, 5.5), jnp.float32),
        "gate_weight": normal_values(keys[2], (LAYERS, D, FF), D ** -0.5, 0.21875, ((1, 32), (2, 2))),
        "up_weight": normal_values(keys[3], (LAYERS, D, FF), D ** -0.5, 0.21875, ((1, 32), (2, 2))),
        "down_weight": normal_values(keys[4], (LAYERS, D, FF), FF ** -0.5, 0.09375, ((1, 32), (2, 2))),
        "norm_gain": jnp.clip(1.0 + 0.1 * jax.random.normal(keys[5], (LAYERS, D), jnp.float32), 0.5, 1.5).astype(jnp.bfloat16),
        "gate_accum": normal_values(keys[6], (LAYERS, D, FF), 2.0, 12.0, ((1, 32), (2, 2)), jnp.float32),
        "up_accum": normal_values(keys[7], (LAYERS, D, FF), 2.0, 12.0, ((1, 32), (2, 2)), jnp.float32),
        "down_accum": normal_values(keys[8], (LAYERS, D, FF), 2.0, 12.0, ((1, 32), (2, 2)), jnp.float32),
        "gain_accum": normal_values(keys[9], (LAYERS, D), 2.0, 12.0, ((1, 32),), jnp.float32),
    }


epsilon = 1e-06

def block_backward(saved_x, cotangent, gate_full, up_full, down_full, gain_full):
    inputs = saved_x.astype(jnp.float32)
    tok_scale = lax.rsqrt(lax.optimization_barrier(jnp.mean(inputs * inputs, axis=1, keepdims=True)) + epsilon)
    whitened = inputs * tok_scale
    gain_vec = gain_full.astype(jnp.float32)
    normed = (whitened * gain_vec).astype(jnp.bfloat16)
    gate_pre = jnp.dot(normed, gate_full, preferred_element_type=jnp.float32)
    up_pre = jnp.dot(normed, up_full, preferred_element_type=jnp.float32)
    sigmoid_gate = jax.nn.sigmoid(gate_pre)
    active = gate_pre * sigmoid_gate
    hidden = (active * up_pre).astype(jnp.bfloat16)
    upstream = cotangent.astype(jnp.bfloat16)
    grad_hidden = jnp.dot(upstream, down_full, preferred_element_type=jnp.float32)
    grad_gate = (grad_hidden * up_pre * (sigmoid_gate * (1.0 + gate_pre * (1.0 - sigmoid_gate)))).astype(jnp.bfloat16)
    grad_up = (grad_hidden * active).astype(jnp.bfloat16)
    grad_normed = jnp.dot(grad_gate, gate_full.T, preferred_element_type=jnp.float32)
    grad_normed = grad_normed + jnp.dot(grad_up, up_full.T, preferred_element_type=jnp.float32)
    grad_white = grad_normed * gain_vec
    inner_mean = lax.optimization_barrier(jnp.mean(grad_white * whitened, axis=1, keepdims=True))
    passed = cotangent + tok_scale * (grad_white - whitened * inner_mean)
    layer_sums = (jnp.dot(normed.T, grad_gate, preferred_element_type=jnp.float32), jnp.dot(normed.T, grad_up, preferred_element_type=jnp.float32), jnp.dot(upstream.T, hidden, preferred_element_type=jnp.float32), lax.optimization_barrier(jnp.sum(grad_normed * whitened, axis=0)))
    return (passed, layer_sums)

def reference(saved_inputs, out_cotangent, gate_weight, up_weight, down_weight, norm_gain, gate_accum, up_accum, down_accum, gain_accum):
    blocks = N_REP * N_FSDP
    cotangent = out_cotangent.reshape(blocks, TOK_DEV, D)
    collected = []
    for layer_index in range(LAYERS - 1, -1, -1):
        gate_full = gate_weight[layer_index]
        up_full = up_weight[layer_index]
        down_full = down_weight[layer_index]
        gain_full = norm_gain[layer_index]

        def layer_step(totals, block_pair):
            passed, layer_sums = block_backward(block_pair[0], block_pair[1], gate_full, up_full, down_full, gain_full)
            summed = (totals[0] + layer_sums[0], totals[1] + layer_sums[1], totals[2] + layer_sums[2], totals[3] + layer_sums[3])
            return (summed, passed)
        start_sums = (jnp.zeros((D, FF), jnp.float32), jnp.zeros((D, FF), jnp.float32), jnp.zeros((D, FF), jnp.float32), jnp.zeros((D,), jnp.float32))
        saved_blocks = saved_inputs[layer_index].reshape(blocks, TOK_DEV, D)
        totals, cotangent = lax.scan(layer_step, start_sums, (saved_blocks, cotangent))
        collected.insert(0, totals)
    gate_grad = gate_accum + jnp.stack([layer_totals[0] for layer_totals in collected])
    up_grad = up_accum + jnp.stack([layer_totals[1] for layer_totals in collected])
    down_grad = down_accum + jnp.stack([layer_totals[2] for layer_totals in collected])
    gain_grad = gain_accum + jnp.stack([layer_totals[3] for layer_totals in collected])
    return (cotangent.reshape(TOKENS, D), gate_grad, up_grad, down_grad, gain_grad)
```

```python
import jax
import jax.numpy as jnp
from jax import lax
from jax.sharding import PartitionSpec as P

epsilon = 1e-06
F32, BF16 = jnp.float32, jnp.bfloat16


N_Y, N_Z = 4, 8


def shift_rep(value, step):
    n = lax.axis_size("rep")
    return lax.ppermute(value, "rep", [(i, (i + step) % n) for i in range(n)])


def swap_tp(value):
    return lax.ppermute(value, "tp", [(0, 1), (1, 0)])


def shift_y(value, step):
    pairs = [(y * N_Z + z, (y + step) % N_Y * N_Z + z) for y in range(N_Y) for z in range(N_Z)]
    return lax.ppermute(value, "fsdp", pairs)


def shift_z(value, step):
    pairs = [(y * N_Z + z, y * N_Z + (z + step) % N_Z) for y in range(N_Y) for z in range(N_Z)]
    return lax.ppermute(value, "fsdp", pairs)


REP_STEPS = (1, 3, 2)


def share_tokens(own):
    moved = {s: shift_rep(own, s) for s in REP_STEPS}
    mine = jnp.stack([own] + [moved[s] for s in range(1, 4)])
    return jnp.concatenate([mine, swap_tp(mine)], axis=0)


def return_tokens(partial, dtype):
    mine = partial[:4] + swap_tp(partial[4:])
    total = mine[0]
    moved = {s: shift_rep(mine[s].astype(dtype), -s) for s in REP_STEPS}
    for s in REP_STEPS:
        total = total + moved[s].astype(F32)
    return total


def scatter_rows(grads, y, z):
    rows_y, rows_z = grads.shape[0] // N_Y, grads.shape[0] // (N_Y * N_Z)

    def part(array, index, rows):
        return lax.dynamic_slice_in_dim(array, index * rows, rows, 0)

    moved = [shift_y(part(grads, (y + s) % N_Y, rows_y).astype(BF16), s) for s in (1, 3, 2)]
    total = part(grads, y, rows_y)
    for m in moved:
        total = total + m.astype(F32)
    moved = [shift_z(part(total, (z + s) % N_Z, rows_z), s) for s in (1, 7, 2, 6, 3, 5, 4)]
    own = part(total, z, rows_z)
    for m in moved:
        own = own + m
    return own


def body(
    saved_inputs,
    out_cotangent,
    gate_weight,
    up_weight,
    down_weight,
    norm_gain,
    gate_accum,
    up_accum,
    down_accum,
    gain_accum,
):
    layers, tokens, d = saved_inputs.shape
    rows, hidden_local = gate_weight.shape[1:]
    n_rep = lax.axis_size("rep")
    q = hidden_local // n_rep
    half = tokens // 2
    r, f, t = lax.axis_index("rep"), lax.axis_index("fsdp"), lax.axis_index("tp")
    y, z = f // N_Z, f % N_Z
    width = -(-(3 * q + 2) // 256) * 256

    def quarter(w):
        return lax.dynamic_slice_in_dim(w, r * q, q, 2)

    packed = jnp.concatenate(
        [quarter(gate_weight), quarter(up_weight), quarter(down_weight), norm_gain[:, :, None],
         jnp.zeros((layers, rows, width - 3 * q - 1), BF16)], axis=2)
    full = {l: lax.all_gather(packed[l], "fsdp", axis=0, tiled=True) for l in range(layers - 1, -1, -1)}

    own_x = lax.dynamic_slice_in_dim(saved_inputs, t * half, half, 1)
    cotangent = lax.dynamic_slice_in_dim(out_cotangent, t * half, half, 0)
    top = share_tokens(jnp.stack([own_x[layers - 1], cotangent.astype(BF16)]))
    x_all, u_all = top[:, 0], top[:, 1]
    lower = {l: share_tokens(own_x[l]) for l in range(layers - 1)}
    rows_first = (((0,), (0,)), ((), ()))
    cols = (((1,), (1,)), ((), ()))

    shards = {}
    for l in range(layers - 1, -1, -1):
        w = full[l]
        gate_w, up_w, down_w = w[:, :q], w[:, q : 2 * q], w[:, 2 * q : 3 * q]
        gain = w[:, 3 * q].astype(F32)
        x = x_all.reshape(8 * half, d).astype(F32)
        u = u_all.reshape(8 * half, d)
        scale = lax.rsqrt(jnp.mean(x * x, axis=1, keepdims=True) + epsilon)
        white = x * scale
        normed = (white * gain).astype(BF16)
        gate_pre = jnp.dot(normed, gate_w, preferred_element_type=F32)
        up_pre = jnp.dot(normed, up_w, preferred_element_type=F32)
        sig = jax.nn.sigmoid(gate_pre)
        active = gate_pre * sig
        hidden = (active * up_pre).astype(BF16)
        grad_hidden = jnp.dot(u, down_w, preferred_element_type=F32)
        grad_gate = (grad_hidden * up_pre * (sig * (1.0 + gate_pre * (1.0 - sig)))).astype(BF16)
        grad_up = (grad_hidden * active).astype(BF16)
        partial = lax.dot_general(grad_gate, gate_w, cols, preferred_element_type=F32)
        partial = partial + lax.dot_general(grad_up, up_w, cols, preferred_element_type=F32)
        grad_normed = return_tokens(partial.reshape(8, half, d), F32)

        own = own_x[l].astype(F32)
        own_scale = lax.rsqrt(jnp.mean(own * own, axis=1, keepdims=True) + epsilon)
        own_white = own * own_scale
        grad_white = grad_normed * gain
        inner = jnp.mean(grad_white * own_white, axis=1, keepdims=True)
        cotangent = cotangent + own_scale * (grad_white - own_white * inner)
        if l:
            x_all, u_all = lower[l - 1], share_tokens(cotangent.astype(BF16))

        gain_part = jnp.sum(partial * white, axis=0)
        gain_high = gain_part.astype(BF16).astype(F32)
        gate_g = lax.dot_general(normed, grad_gate, rows_first, preferred_element_type=F32)
        up_g = lax.dot_general(normed, grad_up, rows_first, preferred_element_type=F32)
        down_g = lax.dot_general(u, hidden, rows_first, preferred_element_type=F32)
        grads = jnp.concatenate(
            [gate_g, up_g, down_g, gain_high[:, None], (gain_part - gain_high)[:, None],
             jnp.zeros((d, width - 3 * q - 2), F32)], axis=1)
        shard = scatter_rows(grads, y, z)
        moved = {s: shift_rep(shard, s) for s in REP_STEPS}
        shards[l] = jnp.stack([shard] + [moved[s] for s in range(1, n_rep)])

    def gathered(l, which):
        return jnp.concatenate(
            [lax.dynamic_index_in_dim(shards[l], (r - k) % n_rep, 0, False)[:, which * q : (which + 1) * q]
             for k in range(n_rep)], axis=1)

    outs = [jnp.stack([acc[l] + gathered(l, i) for l in range(layers)])
            for i, acc in enumerate((gate_accum, up_accum, down_accum))]
    gain_half = jnp.stack([jnp.sum(shards[l][:, :, 3 * q : 3 * q + 2], axis=(0, 2)) for l in range(layers)])
    gain_grad = gain_accum + gain_half + swap_tp(gain_half)

    other = swap_tp(cotangent)
    both = jnp.stack([cotangent, other])
    cot_out = jnp.concatenate([lax.dynamic_index_in_dim(both, t, 0, False),
                               lax.dynamic_index_in_dim(both, 1 - t, 0, False)], axis=0)
    return (cot_out, outs[0], outs[1], outs[2], gain_grad)


def solution(mesh):
    return jax.shard_map(
        body,
        mesh=mesh,
        in_specs=(
            P(None, ("rep", "fsdp"), None),
            P(("rep", "fsdp"), None),
            P(None, "fsdp", "tp"),
            P(None, "fsdp", "tp"),
            P(None, "fsdp", "tp"),
            P(None, "fsdp"),
            P(None, "fsdp", "tp"),
            P(None, "fsdp", "tp"),
            P(None, "fsdp", "tp"),
            P(None, "fsdp"),
        ),
        out_specs=(
            P(("rep", "fsdp"), None),
            P(None, "fsdp", "tp"),
            P(None, "fsdp", "tp"),
            P(None, "fsdp", "tp"),
            P(None, "fsdp"),
        ),
        check_vma=False,
    )
```

```python
import functools

import jax
import jax.numpy as jnp
from jax import lax
from jax.experimental import pallas as pl
from jax.experimental.pallas import tpu as pltpu
from jax.sharding import PartitionSpec as P

epsilon = 1e-06
F32, BF16 = jnp.float32, jnp.bfloat16


N_Y, N_Z, N_REP = 4, 8, 4
REP_STEPS = (1, 3, 2)
Y_STEPS = (1, 3, 2)
Z_STEPS = (4, 3, 5, 2, 6, 1, 7)
VMEM = pl.BlockSpec(memory_space=pltpu.VMEM)
SMEM = pl.BlockSpec(memory_space=pltpu.SMEM)


def shift_rep(value, step):
    return lax.ppermute(value, "rep", [(i, (i + step) % N_REP) for i in range(N_REP)])


def swap_tp(value):
    return lax.ppermute(value, "tp", [(0, 1), (1, 0)])


def shift_y(value, step):
    pairs = [(y * N_Z + z, (y + step) % N_Y * N_Z + z) for y in range(N_Y) for z in range(N_Z)]
    return lax.ppermute(value, "fsdp", pairs)


def shift_z(value, step):
    pairs = [(y * N_Z + z, y * N_Z + (z + step) % N_Z) for y in range(N_Y) for z in range(N_Z)]
    return lax.ppermute(value, "fsdp", pairs)


def place_kernel(n, me_ref, *refs):
    out_ref = refs[n]
    for s in range(n):
        out_ref[lax.rem(me_ref[0] + (n - s), n)] = refs[s][...]


def place(me, pieces):
    n = len(pieces)
    return pl.pallas_call(
        functools.partial(place_kernel, n),
        out_shape=jax.ShapeDtypeStruct((n,) + pieces[0].shape, pieces[0].dtype),
        in_specs=[SMEM] + [VMEM] * n,
        out_specs=VMEM,
        cost_estimate=pl.CostEstimate(flops=1000000, bytes_accessed=2 * n * pieces[0].size * 2, transcendentals=0),
        name="place",
    )(me.reshape(1), *pieces)


def gather_weights(packed, y, z):
    rows, width = packed.shape
    moved = {s: shift_z(packed, s) for s in Z_STEPS}
    line = place(z, [packed] + [moved[s] for s in range(1, N_Z)]).reshape(N_Z * rows, width)
    moved = {s: shift_y(line, s) for s in Y_STEPS}
    return place(y, [line] + [moved[s] for s in range(1, N_Y)]).reshape(N_Y * N_Z * rows, width)


def share_tokens(own):
    moved = {s: shift_rep(own, s) for s in REP_STEPS}
    mine = jnp.stack([own] + [moved[s] for s in range(1, N_REP)])
    return jnp.concatenate([mine, swap_tp(mine)], axis=0)


def return_tokens(partial):
    mine = partial[:4] + swap_tp(partial[4:])
    total = mine[0]
    moved = {s: shift_rep(mine[s], -s) for s in REP_STEPS}
    for s in REP_STEPS:
        total = total + moved[s]
    return total


def grads_kernel(rows, block, y_ref, normed_ref, u_ref, gg_ref, gu_ref, hid_ref, extra_ref, o0, o1, o2, o3, acc):
    contract = (((0,), (0,)), ((), ()))
    outs = (o0, o1, o2, o3)
    for i, (left, right) in enumerate(((normed_ref, gg_ref), (normed_ref, gu_ref), (u_ref, hid_ref))):
        product = lax.dot_general(left[...], right[...], contract, preferred_element_type=F32)
        acc[...] = product
        if i == 0:
            acc[:, block - 128 :] += extra_ref[...]
        for s in range(N_Y):
            start = pl.multiple_of(lax.rem(y_ref[0] + s, N_Y) * rows, rows)
            outs[s][:, i * block : (i + 1) * block] = acc[pl.ds(start, rows), :].astype(BF16)


def weight_grads(y, normed, u, gg, gu, hid, extra):
    tokens, d = normed.shape
    block = gg.shape[1]
    rows = d // N_Y
    return pl.pallas_call(
        functools.partial(grads_kernel, rows, block),
        out_shape=[jax.ShapeDtypeStruct((rows, 3 * block), BF16)] * N_Y,
        in_specs=[SMEM] + [VMEM] * 6,
        out_specs=[VMEM] * N_Y,
        scratch_shapes=[pltpu.VMEM((d, block), F32)],
        cost_estimate=pl.CostEstimate(flops=6 * tokens * d * block, bytes_accessed=10000000, transcendentals=0),
        compiler_params=pltpu.CompilerParams(vmem_limit_bytes=48 * 1024 * 1024),
        name="weight_grads",
    )(y.reshape(1), normed, u, gg, gu, hid, extra)


def scatter_rows(blocks, z):
    moved = [shift_y(blocks[s], s) for s in Y_STEPS]
    total = blocks[0].astype(F32)
    for m in moved:
        total = total + m.astype(F32)
    rows = total.shape[0] // N_Z

    def part(index):
        return lax.dynamic_slice_in_dim(total, index * rows, rows, 0)

    moved = [shift_z(part((z + s) % N_Z), s) for s in Z_STEPS]
    own = part(z)
    for m in moved:
        own = own + m
    return own


def finish_kernel(q, block, r_ref, b0, b1, b2, b3, gate_ref, up_ref, down_ref, go, uo, do, stack):
    for s, b in enumerate((b0, b1, b2, b3)):
        stack[lax.rem(r_ref[0] + (N_REP - s), N_REP)] = b[...]
    for i, (acc, out) in enumerate(((gate_ref, go), (up_ref, uo), (down_ref, do))):
        whole = jnp.concatenate([stack[k, :, i * block : i * block + q] for k in range(N_REP)], axis=1)
        out[...] = acc[...] + whole


def finish(r, blocks, gate, up, down, q, block):
    shape = jax.ShapeDtypeStruct(gate.shape, F32)
    return pl.pallas_call(
        functools.partial(finish_kernel, q, block),
        out_shape=[shape] * 3,
        in_specs=[SMEM] + [VMEM] * 7,
        out_specs=[VMEM] * 3,
        scratch_shapes=[pltpu.VMEM((N_REP,) + blocks[0].shape, F32)],
        cost_estimate=pl.CostEstimate(flops=1000000, bytes_accessed=2000000, transcendentals=0),
        name="finish",
    )(r.reshape(1), *blocks, gate, up, down)


def body(
    saved_inputs,
    out_cotangent,
    gate_weight,
    up_weight,
    down_weight,
    norm_gain,
    gate_accum,
    up_accum,
    down_accum,
    gain_accum,
):
    layers, tokens, d = saved_inputs.shape
    rows, hidden_local = gate_weight.shape[1:]
    q = hidden_local // N_REP
    block = -(-(q + 2) // 128) * 128
    half = tokens // 2
    r, f, t = lax.axis_index("rep"), lax.axis_index("fsdp"), lax.axis_index("tp")
    y, z = f // N_Z, f % N_Z

    def quarter(w):
        return lax.dynamic_slice_in_dim(w, r * q, q, 1)

    def pack(l):
        pad = jnp.zeros((rows, block - q), BF16)
        tail = jnp.concatenate([norm_gain[l][:, None], pad[:, 1:]], axis=1)
        return jnp.concatenate(
            [quarter(gate_weight[l]), tail, quarter(up_weight[l]), pad, quarter(down_weight[l]), pad], axis=1)

    own_x = lax.dynamic_slice_in_dim(saved_inputs, t * half, half, 1)
    cotangent = lax.dynamic_slice_in_dim(out_cotangent, t * half, half, 0)

    full = {layers - 1: gather_weights(pack(layers - 1), y, z)}
    top = share_tokens(jnp.stack([own_x[layers - 1], cotangent.astype(BF16)]))
    x_all, u_all = top[:, 0], top[:, 1]
    for l in range(layers - 2, -1, -1):
        full[l] = gather_weights(pack(l), y, z)
    lower = {l: share_tokens(own_x[l]) for l in range(layers - 1)}
    cols = (((1,), (1,)), ((), ()))

    finished, gain_half = {}, {}
    for l in range(layers - 1, -1, -1):
        w = full[l]
        gate_w, up_w, down_w = w[:, :block], w[:, block : 2 * block], w[:, 2 * block :]
        gain = w[:, q].astype(F32)
        x = x_all.reshape(8 * half, d).astype(F32)
        u = u_all.reshape(8 * half, d)
        scale = lax.rsqrt(jnp.mean(x * x, axis=1, keepdims=True) + epsilon)
        white = x * scale
        normed = (white * gain).astype(BF16)
        gate_pre = jnp.dot(normed, gate_w, preferred_element_type=F32)
        up_pre = jnp.dot(normed, up_w, preferred_element_type=F32)
        sig = jax.nn.sigmoid(gate_pre)
        active = gate_pre * sig
        hidden = (active * up_pre).astype(BF16)
        grad_hidden = jnp.dot(u, down_w, preferred_element_type=F32)
        grad_gate = (grad_hidden * up_pre * (sig * (1.0 + gate_pre * (1.0 - sig)))).astype(BF16)
        grad_up = (grad_hidden * active).astype(BF16)
        partial = lax.dot_general(grad_gate, gate_w, cols, preferred_element_type=F32)
        partial = partial + lax.dot_general(grad_up, up_w, cols, preferred_element_type=F32)
        grad_normed = return_tokens(partial.reshape(8, half, d))

        own = own_x[l].astype(F32)
        own_scale = lax.rsqrt(jnp.mean(own * own, axis=1, keepdims=True) + epsilon)
        own_white = own * own_scale
        grad_white = grad_normed * gain
        inner = jnp.mean(grad_white * own_white, axis=1, keepdims=True)
        cotangent = cotangent + own_scale * (grad_white - own_white * inner)
        if l:
            x_all, u_all = lower[l - 1], share_tokens(cotangent.astype(BF16))

        gain_part = jnp.sum(partial * white, axis=0)
        gain_high = gain_part.astype(BF16).astype(F32)
        lane = lax.broadcasted_iota(jnp.int32, (d, 128), 1) - (q - block + 128)
        extra = jnp.where(lane == 0, gain_high[:, None], jnp.where(lane == 1, (gain_part - gain_high)[:, None], 0.0))
        shard = scatter_rows(weight_grads(y, normed, u, grad_gate, grad_up, hidden, extra), z)
        moved = {s: shift_rep(shard, s) for s in REP_STEPS}
        blocks = [shard] + [moved[s] for s in range(1, N_REP)]
        finished[l] = finish(r, blocks, gate_accum[l], up_accum[l], down_accum[l], q, block)
        gain_half[l] = sum(jnp.sum(b[:, q : q + 2], axis=1) for b in blocks)

    outs = [jnp.stack([finished[l][i] for l in range(layers)]) for i in range(3)]
    gain_sum = jnp.stack([gain_half[l] for l in range(layers)])
    gain_grad = gain_accum + gain_sum + swap_tp(gain_sum)

    other = swap_tp(cotangent)
    both = jnp.stack([cotangent, other])
    cot_out = jnp.concatenate([lax.dynamic_index_in_dim(both, t, 0, False),
                               lax.dynamic_index_in_dim(both, 1 - t, 0, False)], axis=0)
    return (cot_out, outs[0], outs[1], outs[2], gain_grad)


def solution(mesh):
    return jax.shard_map(
        body,
        mesh=mesh,
        in_specs=(
            P(None, ("rep", "fsdp"), None),
            P(("rep", "fsdp"), None),
            P(None, "fsdp", "tp"),
            P(None, "fsdp", "tp"),
            P(None, "fsdp", "tp"),
            P(None, "fsdp"),
            P(None, "fsdp", "tp"),
            P(None, "fsdp", "tp"),
            P(None, "fsdp", "tp"),
            P(None, "fsdp"),
        ),
        out_specs=(
            P(("rep", "fsdp"), None),
            P(None, "fsdp", "tp"),
            P(None, "fsdp", "tp"),
            P(None, "fsdp", "tp"),
            P(None, "fsdp"),
        ),
        check_vma=False,
    )
```

```python
import functools

import jax
import jax.numpy as jnp
from jax import lax
from jax.experimental import pallas as pl
from jax.experimental.pallas import tpu as pltpu
from jax.sharding import PartitionSpec as P

epsilon = 1e-06
F32, BF16 = jnp.float32, jnp.bfloat16


N_Y, N_Z, N_REP = 4, 8, 4
REP_STEPS = (1, 3, 2)
Y_STEPS = (1, 3, 2)
Z_STEPS = (4, 3, 5, 2, 6, 1, 7)
VMEM = pl.BlockSpec(memory_space=pltpu.VMEM)
SMEM = pl.BlockSpec(memory_space=pltpu.SMEM)


def shift_rep(value, step):
    return lax.ppermute(value, "rep", [(i, (i + step) % N_REP) for i in range(N_REP)])


def swap_tp(value):
    return lax.ppermute(value, "tp", [(0, 1), (1, 0)])


def shift_y(value, step):
    pairs = [(y * N_Z + z, (y + step) % N_Y * N_Z + z) for y in range(N_Y) for z in range(N_Z)]
    return lax.ppermute(value, "fsdp", pairs)


def shift_z(value, step):
    pairs = [(y * N_Z + z, y * N_Z + (z + step) % N_Z) for y in range(N_Y) for z in range(N_Z)]
    return lax.ppermute(value, "fsdp", pairs)


Y_GROUPS = [[y * N_Z + z for y in range(N_Y)] for z in range(N_Z)]
Z_GROUPS = [[y * N_Z + z for z in range(N_Z)] for y in range(N_Y)]


def exchange(value, axis, groups=None):
    return lax.all_to_all(value, axis, 0, 0, tiled=True, axis_index_groups=groups)


def after(value, *others):
    return lax.optimization_barrier((value, others))[0]


def pack_kernel(q, block, r_ref, gate_ref, up_ref, down_ref, gain_ref, *outs):
    for l, out in enumerate(outs):
        out[...] = jnp.zeros_like(out)
        out[:, q : q + 1] = gain_ref[l]
    for k in range(N_REP):

        @pl.when(r_ref[0] == k)
        def _():
            for l, out in enumerate(outs):
                for i, w in enumerate((gate_ref, up_ref, down_ref)):
                    out[:, i * block : i * block + q] = w[l, :, k * q : (k + 1) * q]


def pack(r, gate, up, down, gain, q, block):
    layers, rows, _ = gate.shape
    return pl.pallas_call(
        functools.partial(pack_kernel, q, block),
        out_shape=[jax.ShapeDtypeStruct((rows, 3 * block), BF16)] * layers,
        in_specs=[SMEM] + [VMEM] * 4,
        out_specs=[VMEM] * layers,
        cost_estimate=pl.CostEstimate(flops=1000000, bytes_accessed=1000000, transcendentals=0),
        name="pack",
    )(r.reshape(1), gate, up, down, gain[:, :, None])


def place_kernel(n, me_ref, *refs):
    out_ref = refs[n]
    for s in range(n):
        out_ref[lax.rem(me_ref[0] + (n - s), n)] = refs[s][...]


def place(me, pieces):
    n = len(pieces)
    return pl.pallas_call(
        functools.partial(place_kernel, n),
        out_shape=jax.ShapeDtypeStruct((n,) + pieces[0].shape, pieces[0].dtype),
        in_specs=[SMEM] + [VMEM] * n,
        out_specs=VMEM,
        cost_estimate=pl.CostEstimate(flops=1000000, bytes_accessed=2 * n * pieces[0].size * 2, transcendentals=0),
        name="place",
    )(me.reshape(1), *pieces)


def share_tokens(own):
    moved = {s: shift_rep(own, s) for s in REP_STEPS}
    mine = jnp.stack([own] + [moved[s] for s in range(1, N_REP)])
    swapped = swap_tp(mine)
    return jnp.concatenate([mine, swapped], axis=0)


def grads_kernel(block, normed_ref, u_ref, gg_ref, gu_ref, hid_ref, extra_ref, out):
    contract = (((0,), (0,)), ((), ()))
    for i, (left, right) in enumerate(((normed_ref, gg_ref), (normed_ref, gu_ref), (u_ref, hid_ref))):
        product = lax.dot_general(left[...], right[...], contract, preferred_element_type=F32)
        if i == 0:
            out[:, : block - 128] = product[:, : block - 128].astype(BF16)
            out[:, block - 128 : block] = (product[:, block - 128 :] + extra_ref[...]).astype(BF16)
        else:
            out[:, i * block : (i + 1) * block] = product.astype(BF16)


def weight_grads(normed, u, gg, gu, hid, extra):
    tokens, d = normed.shape
    block = gg.shape[1]
    return pl.pallas_call(
        functools.partial(grads_kernel, block),
        out_shape=jax.ShapeDtypeStruct((d, 3 * block), BF16),
        in_specs=[VMEM] * 6,
        out_specs=VMEM,
        cost_estimate=pl.CostEstimate(flops=6 * tokens * d * block, bytes_accessed=10000000, transcendentals=0),
        compiler_params=pltpu.CompilerParams(vmem_limit_bytes=48 * 1024 * 1024),
        name="weight_grads",
    )(normed, u, gg, gu, hid, extra)


def finish_kernel(q, block, layer, r_ref, b0, b1, b2, b3, *refs):
    accums, done, outs, stack = refs[:3], refs[3:-4], refs[-4:-1], refs[-1]
    for s, b in enumerate((b0, b1, b2, b3)):
        stack[lax.rem(r_ref[0] + (N_REP - s), N_REP)] = b[...]
    for i in range(3):
        whole = jnp.concatenate([stack[k, :, i * block : i * block + q] for k in range(N_REP)], axis=1)
        if done:
            outs[i][layer] = accums[i][layer] + whole
            outs[i][1 - layer] = done[i][...]
        else:
            outs[i][...] = accums[i][layer] + whole


def finish(r, pieces, layer, accums, done, q, block):
    shape = accums[0].shape if done else accums[0].shape[1:]
    return pl.pallas_call(
        functools.partial(finish_kernel, q, block, layer),
        out_shape=[jax.ShapeDtypeStruct(shape, F32)] * 3,
        in_specs=[SMEM] + [VMEM] * (7 + len(done)),
        out_specs=[VMEM] * 3,
        scratch_shapes=[pltpu.VMEM((N_REP,) + pieces[0].shape, F32)],
        cost_estimate=pl.CostEstimate(flops=1000000, bytes_accessed=2000000, transcendentals=0),
        name="finish",
    )(r.reshape(1), *pieces, *accums, *done)


def body(
    saved_inputs,
    out_cotangent,
    gate_weight,
    up_weight,
    down_weight,
    norm_gain,
    gate_accum,
    up_accum,
    down_accum,
    gain_accum,
):
    layers, tokens, d = saved_inputs.shape
    rows, hidden_local = gate_weight.shape[1:]
    q = hidden_local // N_REP
    block = -(-(q + 2) // 128) * 128
    half = tokens // 2
    r, f, t = lax.axis_index("rep"), lax.axis_index("fsdp"), lax.axis_index("tp")
    y, z = f // N_Z, f % N_Z

    packed = pack(r, gate_weight, up_weight, down_weight, norm_gain, q, block)
    width = 3 * block
    top, low = layers - 1, 0

    moved = {s: shift_z(packed[top], s) for s in Z_STEPS}
    own_x = lax.dynamic_slice_in_dim(saved_inputs, t * half, half, 1)
    cotangent = lax.dynamic_slice_in_dim(out_cotangent, t * half, half, 0)
    shared = share_tokens(jnp.stack([own_x[top], cotangent.astype(BF16), own_x[low]]))
    line = place(z, [packed[top]] + [moved[s] for s in range(1, N_Z)]).reshape(N_Z * rows, width)
    moved = {s: shift_y(line, s) for s in Y_STEPS}
    full_top = place(y, [line] + [moved[s] for s in range(1, N_Y)]).reshape(d, width)

    low_packed = after(packed[low], line)
    line = exchange(jnp.broadcast_to(low_packed[None], (N_Z, rows, width)), "fsdp", Z_GROUPS)
    line = after(line.reshape(1, N_Z * rows, width), full_top)
    full_low = exchange(jnp.broadcast_to(line, (N_Y, N_Z * rows, width)), "fsdp", Y_GROUPS).reshape(d, width)

    cols = (((1,), (1,)), ((), ()))
    pick = (lax.broadcasted_iota(jnp.int32, (8, block), 1) == q).astype(BF16)

    def forward(x, u, w):
        gate_w, up_w, down_w = w[:, :block], w[:, block : 2 * block], w[:, 2 * block :]
        gain = lax.dot_general(pick, gate_w, cols, preferred_element_type=F32)[0]
        x = x.reshape(8 * half, d).astype(F32)
        u = u.reshape(8 * half, d)
        scale = lax.rsqrt(jnp.mean(x * x, axis=1, keepdims=True) + epsilon)
        white = x * scale
        normed = (white * gain).astype(BF16)
        gate_pre = jnp.dot(normed, gate_w, preferred_element_type=F32)
        up_pre = jnp.dot(normed, up_w, preferred_element_type=F32)
        sig = jax.nn.sigmoid(gate_pre)
        active = gate_pre * sig
        hidden = (active * up_pre).astype(BF16)
        grad_hidden = jnp.dot(u, down_w, preferred_element_type=F32)
        grad_gate = (grad_hidden * up_pre * (sig * (1.0 + gate_pre * (1.0 - sig)))).astype(BF16)
        grad_up = (grad_hidden * active).astype(BF16)
        return gain, white, normed, u, hidden, grad_gate, grad_up

    def to_normed(grad_gate, grad_up, w):
        partial = lax.dot_general(grad_gate, w[:, :block], cols, preferred_element_type=F32)
        return partial + lax.dot_general(grad_up, w[:, block : 2 * block], cols, preferred_element_type=F32)

    def gain_columns(partial, white):
        gain_part = jnp.sum(partial * white, axis=0)
        gain_high = gain_part.astype(BF16).astype(F32)
        lane = lax.broadcasted_iota(jnp.int32, (d, 128), 1) - (q - block + 128)
        return jnp.where(lane == 0, gain_high[:, None], jnp.where(lane == 1, (gain_part - gain_high)[:, None], 0.0))

    def step_back(cotangent, own_x, grad_normed, gain):
        own = own_x.astype(F32)
        own_scale = lax.rsqrt(jnp.mean(own * own, axis=1, keepdims=True) + epsilon)
        own_white = own * own_scale
        grad_white = grad_normed * gain
        inner = jnp.mean(grad_white * own_white, axis=1, keepdims=True)
        return cotangent + own_scale * (grad_white - own_white * inner)

    gain, white, normed, u, hidden, gg, gu = forward(shared[:, 0], shared[:, 1], full_top)
    partial = to_normed(gg, gu, full_top).reshape(8, half, d)
    mine = partial[:4] + swap_tp(partial[4:])
    moved = {s: shift_rep(mine[s], -s) for s in REP_STEPS}
    extra = gain_columns(partial.reshape(8 * half, d), white)
    grads_top = weight_grads(after(normed, mine), u, gg, gu, hidden, extra)
    received = exchange(grads_top.reshape(N_Y, N_Z * rows, width), "fsdp", Y_GROUPS)
    grad_normed = mine[0]
    for s in REP_STEPS:
        grad_normed = grad_normed + moved[s]
    cotangent = step_back(cotangent, own_x[top], grad_normed, gain)

    u_low = share_tokens(cotangent.astype(BF16))
    full_low = after(full_low, grads_top)
    gain, white, normed, u, hidden, gg, gu = forward(shared[:, 2], u_low, full_low)
    partial = to_normed(gg, gu, full_low).reshape(8, half, d)
    extra = gain_columns(partial.reshape(8 * half, d), white)
    grads_low = weight_grads(normed, u, gg, gu, hidden, extra)
    blocks = grads_low.reshape(N_Y, N_Z * rows, width)
    moved_y = {s: shift_y(lax.dynamic_index_in_dim(blocks, (y + s) % N_Y, 0, False), s) for s in Y_STEPS}
    own_y = lax.dynamic_index_in_dim(blocks, y, 0, False)

    partial = after(partial, grads_low)
    mine = partial[:4] + swap_tp(partial[4:])
    moved = {s: shift_rep(mine[s], -s) for s in REP_STEPS}
    grad_normed = mine[0]
    for s in REP_STEPS:
        grad_normed = grad_normed + moved[s]
    cotangent = step_back(cotangent, own_x[low], grad_normed, gain)

    received = after(received, grads_low)
    total = jnp.sum(received.astype(F32), axis=0)
    shard_in = total.reshape(N_Z, rows, width)
    shard_top = jnp.sum(exchange(shard_in, "fsdp", Z_GROUPS), axis=0)
    total = own_y.astype(F32)
    ready = after(moved_y, shard_in, mine)
    for s in Y_STEPS:
        total = total + ready[s].astype(F32)
    total = total.reshape(N_Z, rows, width)
    moved_z = {s: shift_z(lax.dynamic_index_in_dim(total, (z + s) % N_Z, 0, False), s) for s in Z_STEPS}
    shard_low = lax.dynamic_index_in_dim(total, z, 0, False)
    for s in Z_STEPS:
        shard_low = shard_low + moved_z[s]

    accums = (gate_accum, up_accum, down_accum)
    outs, gain_half = (), {}
    for l, shard in ((top, after(shard_top, total)), (low, shard_low)):
        moved = {s: shift_rep(shard, s) for s in REP_STEPS}
        pieces = [shard] + [moved[s] for s in range(1, N_REP)]
        outs = finish(r, pieces, l, accums, tuple(outs), q, block)
        gain_half[l] = sum(jnp.sum(b[:, q : q + 2], axis=1) for b in pieces)

    gain_sum = jnp.stack([gain_half[l] for l in range(layers)])
    gain_grad = gain_accum + gain_sum + swap_tp(gain_sum)

    other = swap_tp(cotangent)
    both = jnp.stack([cotangent, other])
    cot_out = jnp.concatenate([lax.dynamic_index_in_dim(both, t, 0, False),
                               lax.dynamic_index_in_dim(both, 1 - t, 0, False)], axis=0)
    return (cot_out, outs[0], outs[1], outs[2], gain_grad)


def solution(mesh):
    return jax.shard_map(
        body,
        mesh=mesh,
        in_specs=(
            P(None, ("rep", "fsdp"), None),
            P(("rep", "fsdp"), None),
            P(None, "fsdp", "tp"),
            P(None, "fsdp", "tp"),
            P(None, "fsdp", "tp"),
            P(None, "fsdp"),
            P(None, "fsdp", "tp"),
            P(None, "fsdp", "tp"),
            P(None, "fsdp", "tp"),
            P(None, "fsdp"),
        ),
        out_specs=(
            P(("rep", "fsdp"), None),
            P(None, "fsdp", "tp"),
            P(None, "fsdp", "tp"),
            P(None, "fsdp", "tp"),
            P(None, "fsdp"),
        ),
        check_vma=False,
    )
```

```python
import functools

import jax
import jax.numpy as jnp
from jax import lax
from jax.experimental import pallas as pl
from jax.experimental.pallas import tpu as pltpu
from jax.sharding import PartitionSpec as P

epsilon = 1e-06
F32, BF16, F16 = jnp.float32, jnp.bfloat16, jnp.float16


N_Y, N_Z, N_REP = 4, 8, 4
REP_STEPS = (1, 3, 2)
Y_STEPS = (1, 3, 2)
VMEM = pl.BlockSpec(memory_space=pltpu.VMEM)
SMEM = pl.BlockSpec(memory_space=pltpu.SMEM)


def shift_rep(value, step):
    return lax.ppermute(value, "rep", [(i, (i + step) % N_REP) for i in range(N_REP)])


def swap_tp(value):
    return lax.ppermute(value, "tp", [(0, 1), (1, 0)])


def shift_y(value, step):
    pairs = [(y * N_Z + z, (y + step) % N_Y * N_Z + z) for y in range(N_Y) for z in range(N_Z)]
    return lax.ppermute(value, "fsdp", pairs)


Y_GROUPS = [[y * N_Z + z for y in range(N_Y)] for z in range(N_Z)]
Z_GROUPS = [[y * N_Z + z for z in range(N_Z)] for y in range(N_Y)]


def exchange(value, axis, groups=None):
    return lax.all_to_all(value, axis, 0, 0, tiled=True, axis_index_groups=groups)


def after(value, *others):
    return lax.optimization_barrier((value, others))[0]


def pack_kernel(q, block, r_ref, gate_ref, up_ref, down_ref, gain_ref, *outs):
    for l, out in enumerate(outs):
        out[...] = jnp.zeros_like(out)
        out[:, q : q + 1] = gain_ref[l]
    for k in range(N_REP):

        @pl.when(r_ref[0] == k)
        def _():
            for l, out in enumerate(outs):
                for i, w in enumerate((gate_ref, up_ref, down_ref)):
                    out[:, i * block : i * block + q] = w[l, :, k * q : (k + 1) * q]


def pack(r, gate, up, down, gain, q, block):
    layers, rows, _ = gate.shape
    return pl.pallas_call(
        functools.partial(pack_kernel, q, block),
        out_shape=[jax.ShapeDtypeStruct((rows, 3 * block), BF16)] * layers,
        in_specs=[SMEM] + [VMEM] * 4,
        out_specs=[VMEM] * layers,
        cost_estimate=pl.CostEstimate(flops=1000000, bytes_accessed=1000000, transcendentals=0),
        name="pack",
    )(r.reshape(1), gate, up, down, gain[:, :, None])


def place_kernel(n, me_ref, *refs):
    out_ref = refs[n]
    for s in range(n):
        out_ref[lax.rem(me_ref[0] + (n - s), n)] = refs[s][...]


def place(me, pieces):
    n = len(pieces)
    return pl.pallas_call(
        functools.partial(place_kernel, n),
        out_shape=jax.ShapeDtypeStruct((n,) + pieces[0].shape, pieces[0].dtype),
        in_specs=[SMEM] + [VMEM] * n,
        out_specs=VMEM,
        cost_estimate=pl.CostEstimate(flops=1000000, bytes_accessed=2 * n * pieces[0].size * 2, transcendentals=0),
        name="place",
    )(me.reshape(1), *pieces)


def share_tokens(own, *others):
    moved = {s: shift_rep(own, s) for s in REP_STEPS}
    if others:
        moved = after(moved, *others)
    mine = jnp.stack([own] + [moved[s] for s in range(1, N_REP)])
    swapped = swap_tp(mine)
    return jnp.concatenate([mine, swapped], axis=0)


def products(block, normed_ref, u_ref, gg_ref, gu_ref, hid_ref, extra_ref, write):
    contract = (((0,), (0,)), ((), ()))
    for i, (left, right) in enumerate(((normed_ref, gg_ref), (normed_ref, gu_ref), (u_ref, hid_ref))):
        product = lax.dot_general(left[...], right[...], contract, preferred_element_type=F32)
        if i == 0:
            write(0, block - 128, product[:, : block - 128])
            write(block - 128, block, product[:, block - 128 :] + extra_ref[...])
        else:
            write(i * block, (i + 1) * block, product)


def grads_kernel(block, *refs):
    def write(start, stop, value):
        refs[6][:, start:stop] = value.astype(BF16)

    products(block, *refs[:6], write)


def grads_blocks_kernel(rows, block, y_ref, *refs):
    outs, acc = refs[6:10], refs[10]

    def write(start, stop, value):
        acc[:, : stop - start] = value
        for s in range(N_Y):
            first = pl.multiple_of(lax.rem(y_ref[0] + s, N_Y) * rows, rows)
            outs[s][:, start:stop] = acc[pl.ds(first, rows), : stop - start].astype(outs[s].dtype)

    products(block, *refs[:6], write)


def weight_grads(normed, u, gg, gu, hid, extra, y=None):
    tokens, d = normed.shape
    block = gg.shape[1]
    rows = d // N_Y
    if y is None:
        shapes, kernel, scratch, first = [(d, BF16)], functools.partial(grads_kernel, block), [], ()
    else:
        shapes, kernel = [(rows, F32)] + [(rows, BF16)] * 3, functools.partial(grads_blocks_kernel, rows, block)
        scratch, first = [pltpu.VMEM((d, block), F32)], (y.reshape(1),)
    return pl.pallas_call(
        kernel,
        out_shape=[jax.ShapeDtypeStruct((n, 3 * block), dtype) for n, dtype in shapes],
        in_specs=[SMEM] * len(first) + [VMEM] * 6,
        out_specs=[VMEM] * len(shapes),
        scratch_shapes=scratch,
        cost_estimate=pl.CostEstimate(flops=6 * tokens * d * block, bytes_accessed=10000000, transcendentals=0),
        compiler_params=pltpu.CompilerParams(vmem_limit_bytes=48 * 1024 * 1024),
        name="weight_grads",
    )(*first, normed, u, gg, gu, hid, extra)


def narrow(value, lane):
    most = jnp.max(jnp.abs(value), axis=-1, keepdims=True)
    e = jnp.where(most > 0.0, jnp.clip(jnp.ceil(jnp.log2(most)) - 12.0, -120.0, 120.0), 0.0)
    lanes = lax.broadcasted_iota(jnp.int32, value.shape, value.ndim - 1)
    return jnp.where(lanes == lane, e, value * jnp.exp2(-e)).astype(F16)


def widen(value, lane):
    return value.astype(F32) * jnp.exp2(value[..., lane : lane + 1].astype(F32))


def finish_kernel(q, block, layers, r_ref, b0, b1, b2, b3, *refs):
    accums, outs, stack = refs[:3], refs[3:6], refs[6]
    for s, b in enumerate((b0, b1, b2, b3)):
        stack[lax.rem(r_ref[0] + (N_REP - s), N_REP)] = b[...]
    for l in range(layers):
        for i in range(3):
            whole = jnp.concatenate([stack[k, l, :, i * block : i * block + q] for k in range(N_REP)], axis=1)
            outs[i][l] = accums[i][l] + whole


def finish(r, pieces, accums, q, block):
    return pl.pallas_call(
        functools.partial(finish_kernel, q, block, accums[0].shape[0]),
        out_shape=[jax.ShapeDtypeStruct(accums[0].shape, F32)] * 3,
        in_specs=[SMEM] + [VMEM] * 7,
        out_specs=[VMEM] * 3,
        scratch_shapes=[pltpu.VMEM((N_REP,) + pieces[0].shape, F32)],
        cost_estimate=pl.CostEstimate(flops=1000000, bytes_accessed=2000000, transcendentals=0),
        name="finish",
    )(r.reshape(1), *pieces, *accums)


def token_scale(x):
    x = x.astype(F32)
    return lax.rsqrt(jnp.mean(x * x, axis=1, keepdims=True) + epsilon)


def body(
    saved_inputs,
    out_cotangent,
    gate_weight,
    up_weight,
    down_weight,
    norm_gain,
    gate_accum,
    up_accum,
    down_accum,
    gain_accum,
):
    layers, tokens, d = saved_inputs.shape
    rows, hidden_local = gate_weight.shape[1:]
    q = hidden_local // N_REP
    block = -(-(q + 2) // 128) * 128
    half = tokens // 2
    r, f, t = lax.axis_index("rep"), lax.axis_index("fsdp"), lax.axis_index("tp")
    y = f // N_Z

    packed = pack(r, gate_weight, up_weight, down_weight, norm_gain, q, block)
    width = 3 * block
    top, low = layers - 1, 0

    line = exchange(jnp.broadcast_to(packed[top][None], (N_Z, rows, width)), "fsdp", Z_GROUPS)
    line = line.reshape(N_Z * rows, width)
    own_x = lax.dynamic_slice_in_dim(saved_inputs, t * half, half, 1)
    cotangent = lax.dynamic_slice_in_dim(out_cotangent, t * half, half, 0)
    shared = share_tokens(jnp.stack([own_x[top], cotangent.astype(BF16), own_x[low]]), line)
    moved = {s: shift_y(line, s) for s in Y_STEPS}
    x_top = shared[:, 0].reshape(8 * half, d)
    u_top = shared[:, 1].reshape(8 * half, d)
    scale_top = token_scale(x_top)
    moved = after(moved, u_top, scale_top)
    full_top = place(y, [line] + [moved[s] for s in range(1, N_Y)]).reshape(d, width)

    low_packed = after(packed[low], line)
    line = exchange(jnp.broadcast_to(low_packed[None], (N_Z, rows, width)), "fsdp", Z_GROUPS)
    line_low = line.reshape(N_Z * rows, width)
    cols = (((1,), (1,)), ((), ()))
    pick = (lax.broadcasted_iota(jnp.int32, (8, block), 1) == q).astype(BF16)

    def forward(x, u, w, scale):
        gate_w, up_w, down_w = w[:, :block], w[:, block : 2 * block], w[:, 2 * block :]
        gain = lax.dot_general(pick, gate_w, cols, preferred_element_type=F32)[0]
        white = x.astype(F32) * scale
        normed = (white * gain).astype(BF16)
        gate_pre = jnp.dot(normed, gate_w, preferred_element_type=F32)
        up_pre = jnp.dot(normed, up_w, preferred_element_type=F32)
        sig = jax.nn.sigmoid(gate_pre)
        active = gate_pre * sig
        hidden = (active * up_pre).astype(BF16)
        grad_hidden = jnp.dot(u, down_w, preferred_element_type=F32)
        grad_gate = (grad_hidden * up_pre * (sig * (1.0 + gate_pre * (1.0 - sig)))).astype(BF16)
        grad_up = (grad_hidden * active).astype(BF16)
        return gain, white, normed, hidden, grad_gate, grad_up

    def to_normed(grad_gate, grad_up, w):
        partial = lax.dot_general(grad_gate, w[:, :block], cols, preferred_element_type=F32)
        return partial + lax.dot_general(grad_up, w[:, block : 2 * block], cols, preferred_element_type=F32)

    def gain_columns(partial, white):
        gain_part = jnp.sum(partial * white, axis=0)
        gain_high = gain_part.astype(BF16).astype(F32)
        lane = lax.broadcasted_iota(jnp.int32, (d, 128), 1) - (q - block + 128)
        return jnp.where(lane == 0, gain_high[:, None], jnp.where(lane == 1, (gain_part - gain_high)[:, None], 0.0))

    def step_back(cotangent, own_x, grad_normed, gain):
        own = own_x.astype(F32)
        own_scale = lax.rsqrt(jnp.mean(own * own, axis=1, keepdims=True) + epsilon)
        own_white = own * own_scale
        grad_white = grad_normed * gain
        inner = jnp.mean(grad_white * own_white, axis=1, keepdims=True)
        return cotangent + own_scale * (grad_white - own_white * inner)

    gain, white, normed, hidden, gg, gu = forward(x_top, u_top, full_top, scale_top)
    partial = to_normed(gg, gu, full_top).reshape(8, half, d)
    mine = partial[:4] + swap_tp(partial[4:])
    moved = {s: shift_rep(mine[s], -s) for s in REP_STEPS}
    line_low = after(line_low, mine)
    moved_low = {s: shift_y(line_low, s) for s in Y_STEPS}
    extra = gain_columns(partial.reshape(8 * half, d), white)
    (grads_top,) = weight_grads(after(normed, mine, line_low), u_top, gg, gu, hidden, extra)
    received = exchange(grads_top.reshape(N_Y, N_Z * rows, width), "fsdp", Y_GROUPS)
    grad_normed = mine[0]
    for s in REP_STEPS:
        grad_normed = grad_normed + moved[s]
    cotangent = step_back(cotangent, own_x[top], grad_normed, gain)

    x_low = shared[:, 2].reshape(8 * half, d)
    u_low = share_tokens(cotangent.astype(BF16)).reshape(8 * half, d)
    moved_low, x_low = after((moved_low, x_low), cotangent, grads_top)
    full_low = place(y, [line_low] + [moved_low[s] for s in range(1, N_Y)]).reshape(d, width)
    gain, white, normed, hidden, gg, gu = forward(x_low, u_low, full_low, token_scale(x_low))
    partial = to_normed(gg, gu, full_low).reshape(8, half, d)
    extra = gain_columns(partial.reshape(8 * half, d), white)
    grads_low = weight_grads(normed, u_low, gg, gu, hidden, extra, y)
    moved_y = {s: shift_y(grads_low[s], s) for s in Y_STEPS}

    partial = after(partial, grads_low)
    mine = partial[:4] + swap_tp(partial[4:])
    moved = {s: shift_rep(mine[s], -s) for s in REP_STEPS}
    grad_normed = mine[0]
    for s in REP_STEPS:
        grad_normed = grad_normed + moved[s]
    cotangent = step_back(cotangent, own_x[low], grad_normed, gain)

    received = after(received, grads_low)
    total = jnp.sum(received.astype(F32), axis=0)
    shard_in = narrow(total, q + 2).reshape(N_Z, rows, width)
    shard_top = exchange(shard_in, "fsdp", Z_GROUPS)
    moved_y = after(moved_y, shard_in, mine)
    total = grads_low[0]
    for s in Y_STEPS:
        total = total + moved_y[s].astype(F32)
    shard_in = narrow(total, q + 2).reshape(N_Z, rows, width)
    shard_low = exchange(shard_in, "fsdp", Z_GROUPS)
    own = jnp.stack([narrow(jnp.sum(widen(v, q + 2), axis=0), q + 2) for v in (shard_low, shard_top)])
    moved = {s: shift_rep(own, s) for s in REP_STEPS}
    pieces = [widen(own, q + 2)] + [widen(moved[s], q + 2) for s in range(1, N_REP)]
    outs = finish(r, pieces, (gate_accum, up_accum, down_accum), q, block)
    gain_sum = sum(jnp.sum(b[:, :, q : q + 2], axis=2) for b in pieces)
    gain_grad = gain_accum + gain_sum + swap_tp(gain_sum)

    other = swap_tp(cotangent)
    both = jnp.stack([cotangent, other])
    cot_out = jnp.concatenate([lax.dynamic_index_in_dim(both, t, 0, False),
                               lax.dynamic_index_in_dim(both, 1 - t, 0, False)], axis=0)
    return (cot_out, outs[0], outs[1], outs[2], gain_grad)


def solution(mesh):
    return jax.shard_map(
        body,
        mesh=mesh,
        in_specs=(
            P(None, ("rep", "fsdp"), None),
            P(("rep", "fsdp"), None),
            P(None, "fsdp", "tp"),
            P(None, "fsdp", "tp"),
            P(None, "fsdp", "tp"),
            P(None, "fsdp"),
            P(None, "fsdp", "tp"),
            P(None, "fsdp", "tp"),
            P(None, "fsdp", "tp"),
            P(None, "fsdp"),
        ),
        out_specs=(
            P(("rep", "fsdp"), None),
            P(None, "fsdp", "tp"),
            P(None, "fsdp", "tp"),
            P(None, "fsdp", "tp"),
            P(None, "fsdp"),
        ),
        check_vma=False,
    )
```

```python
import functools

import jax
import jax.numpy as jnp
from jax import lax
from jax.experimental import pallas as pl
from jax.experimental.pallas import tpu as pltpu
from jax.sharding import PartitionSpec as P

epsilon = 1e-06
F32, BF16, F16 = jnp.float32, jnp.bfloat16, jnp.float16


N_Y, N_Z, N_REP = 4, 8, 4
REP_STEPS = (1, 3, 2)
Y_STEPS = (1, 3, 2)
VMEM = pl.BlockSpec(memory_space=pltpu.VMEM)
SMEM = pl.BlockSpec(memory_space=pltpu.SMEM)


def shift_rep(value, step):
    return lax.ppermute(value, "rep", [(i, (i + step) % N_REP) for i in range(N_REP)])


def swap_tp(value):
    return lax.ppermute(value, "tp", [(0, 1), (1, 0)])


def shift_y(value, step):
    pairs = [(y * N_Z + z, (y + step) % N_Y * N_Z + z) for y in range(N_Y) for z in range(N_Z)]
    return lax.ppermute(value, "fsdp", pairs)


Y_GROUPS = [[y * N_Z + z for y in range(N_Y)] for z in range(N_Z)]
Z_GROUPS = [[y * N_Z + z for z in range(N_Z)] for y in range(N_Y)]


def exchange(value, axis, groups=None):
    return lax.all_to_all(value, axis, 0, 0, tiled=True, axis_index_groups=groups)


def after(value, *others):
    return lax.optimization_barrier((value, others))[0]


def pack_kernel(q, block, r_ref, gate_ref, up_ref, down_ref, gain_ref, *refs):
    outs, one = refs[:-1], refs[-1]
    rows = gate_ref.shape[1]
    row = lax.broadcasted_iota(jnp.int32, (rows, rows), 0)
    diagonal = row == lax.broadcasted_iota(jnp.int32, (rows, rows), 1)
    for l, out in enumerate(outs):
        gain = jnp.where(diagonal, gain_ref[l : l + 1].astype(F32), 0.0)
        one[...] = jnp.zeros_like(one)
        one[:, q : q + 1] = jnp.sum(gain, axis=1, keepdims=True).astype(BF16)
        for k in range(N_REP):

            @pl.when(r_ref[0] == k)
            def _():
                for i, w in enumerate((gate_ref, up_ref, down_ref)):
                    one[:, i * block : i * block + q] = w[l, :, k * q : (k + 1) * q]

        for i in range(N_Z):
            out[i] = one[...]


def pack(r, gate, up, down, gain, q, block):
    layers, rows, _ = gate.shape
    return pl.pallas_call(
        functools.partial(pack_kernel, q, block),
        out_shape=[jax.ShapeDtypeStruct((N_Z, rows, 3 * block), BF16)] * layers,
        in_specs=[SMEM] + [VMEM] * 4,
        out_specs=[VMEM] * layers,
        scratch_shapes=[pltpu.VMEM((rows, 3 * block), BF16)],
        cost_estimate=pl.CostEstimate(flops=1000000, bytes_accessed=1000000, transcendentals=0),
        name="pack",
    )(r.reshape(1), gate, up, down, gain)


def place_kernel(n, me_ref, *refs):
    out_ref = refs[n]
    for s in range(n):
        out_ref[lax.rem(me_ref[0] + (n - s), n)] = refs[s][...]


def place(me, pieces):
    n = len(pieces)
    return pl.pallas_call(
        functools.partial(place_kernel, n),
        out_shape=jax.ShapeDtypeStruct((n,) + pieces[0].shape, pieces[0].dtype),
        in_specs=[SMEM] + [VMEM] * n,
        out_specs=VMEM,
        cost_estimate=pl.CostEstimate(flops=1000000, bytes_accessed=2 * n * pieces[0].size * 2, transcendentals=0),
        name="place",
    )(me.reshape(1), *pieces)


def share_tokens(own, *others):
    moved = {s: shift_rep(own, s) for s in REP_STEPS}
    if others:
        moved, own = after((moved, own), *others)
    mine = jnp.stack([own] + [moved[s] for s in range(1, N_REP)])
    swapped = swap_tp(mine)
    return jnp.concatenate([mine, swapped], axis=0)


def products(block, normed_ref, u_ref, gg_ref, gu_ref, hid_ref, extra_ref, write):
    contract = (((0,), (0,)), ((), ()))
    for i, (left, right) in enumerate(((normed_ref, gg_ref), (normed_ref, gu_ref), (u_ref, hid_ref))):
        product = lax.dot_general(left[...], right[...], contract, preferred_element_type=F32)
        if i == 0:
            write(0, block - 128, product[:, : block - 128])
            write(block - 128, block, product[:, block - 128 :] + extra_ref[...])
        else:
            write(i * block, (i + 1) * block, product)


def grads_kernel(block, *refs):
    def write(start, stop, value):
        refs[6][:, start:stop] = value.astype(BF16)

    products(block, *refs[:6], write)


def grads_blocks_kernel(rows, block, y_ref, *refs):
    outs, acc = refs[6:10], refs[10]

    def write(start, stop, value):
        acc[:, : stop - start] = value
        for s in range(N_Y):
            first = pl.multiple_of(lax.rem(y_ref[0] + s, N_Y) * rows, rows)
            outs[s][:, start:stop] = acc[pl.ds(first, rows), : stop - start].astype(outs[s].dtype)

    products(block, *refs[:6], write)


def weight_grads(normed, u, gg, gu, hid, extra, y=None):
    tokens, d = normed.shape
    block = gg.shape[1]
    rows = d // N_Y
    if y is None:
        shapes, kernel, scratch, first = [(d, BF16)], functools.partial(grads_kernel, block), [], ()
    else:
        shapes, kernel = [(rows, F32)] + [(rows, BF16)] * 3, functools.partial(grads_blocks_kernel, rows, block)
        scratch, first = [pltpu.VMEM((d, block), F32)], (y.reshape(1),)
    return pl.pallas_call(
        kernel,
        out_shape=[jax.ShapeDtypeStruct((n, 3 * block), dtype) for n, dtype in shapes],
        in_specs=[SMEM] * len(first) + [VMEM] * 6,
        out_specs=[VMEM] * len(shapes),
        scratch_shapes=scratch,
        cost_estimate=pl.CostEstimate(flops=6 * tokens * d * block, bytes_accessed=10000000, transcendentals=0),
        compiler_params=pltpu.CompilerParams(vmem_limit_bytes=48 * 1024 * 1024),
        name="weight_grads",
    )(*first, normed, u, gg, gu, hid, extra)


def sum_kernel(lane, *refs):
    ins, out_ref = refs[:-1], refs[-1]
    if len(ins) == 1:
        ins = [ins[0].at[i] for i in range(N_Y)]
    total = ins[0][...].astype(F32)
    for m in ins[1:]:
        total = total + m[...].astype(F32)
    most = jnp.max(jnp.abs(total), axis=-1, keepdims=True)
    e = jnp.where(most > 0.0, jnp.clip(jnp.ceil(jnp.log2(most)) - 12.0, -120.0, 120.0), 0.0)
    lanes = lax.broadcasted_iota(jnp.int32, total.shape, 1)
    out_ref[...] = jnp.where(lanes == lane, e, total * jnp.exp2(-e))


def sum_narrow(parts, lane):
    scaled = pl.pallas_call(
        functools.partial(sum_kernel, lane),
        out_shape=jax.ShapeDtypeStruct(parts[0].shape[-2:], F32),
        in_specs=[VMEM] * len(parts),
        out_specs=VMEM,
        cost_estimate=pl.CostEstimate(flops=2000000, bytes_accessed=5000000, transcendentals=0),
        name="sum_narrow",
    )(*parts)
    return scaled.astype(F16)


def narrow(value, lane):
    most = jnp.max(jnp.abs(value), axis=-1, keepdims=True)
    e = jnp.where(most > 0.0, jnp.clip(jnp.ceil(jnp.log2(most)) - 12.0, -120.0, 120.0), 0.0)
    lanes = lax.broadcasted_iota(jnp.int32, value.shape, value.ndim - 1)
    return jnp.where(lanes == lane, e, value * jnp.exp2(-e)).astype(F16)


def widen(value, lane):
    return value.astype(F32) * jnp.exp2(value[..., lane : lane + 1].astype(F32))


def finish_kernel(q, block, layers, r_ref, b0, b1, b2, b3, *refs):
    accums, outs, stack = refs[:3], refs[3:6], refs[6]
    for s, b in enumerate((b0, b1, b2, b3)):
        stack[lax.rem(r_ref[0] + (N_REP - s), N_REP)] = b[...]
    for l in range(layers):
        for i in range(3):
            whole = jnp.concatenate([stack[k, l, :, i * block : i * block + q] for k in range(N_REP)], axis=1)
            outs[i][l] = accums[i][l] + whole


def finish(r, pieces, accums, q, block):
    return pl.pallas_call(
        functools.partial(finish_kernel, q, block, accums[0].shape[0]),
        out_shape=[jax.ShapeDtypeStruct(accums[0].shape, F32)] * 3,
        in_specs=[SMEM] + [VMEM] * 7,
        out_specs=[VMEM] * 3,
        scratch_shapes=[pltpu.VMEM((N_REP,) + pieces[0].shape, F32)],
        cost_estimate=pl.CostEstimate(flops=1000000, bytes_accessed=2000000, transcendentals=0),
        name="finish",
    )(r.reshape(1), *pieces, *accums)


def token_scale(x):
    x = x.astype(F32)
    return lax.rsqrt(jnp.mean(x * x, axis=1, keepdims=True) + epsilon)


def body(
    saved_inputs,
    out_cotangent,
    gate_weight,
    up_weight,
    down_weight,
    norm_gain,
    gate_accum,
    up_accum,
    down_accum,
    gain_accum,
):
    layers, tokens, d = saved_inputs.shape
    rows, hidden_local = gate_weight.shape[1:]
    q = hidden_local // N_REP
    block = -(-(q + 2) // 128) * 128
    half = tokens // 2
    r, f, t = lax.axis_index("rep"), lax.axis_index("fsdp"), lax.axis_index("tp")
    y = f // N_Z

    packed = pack(r, gate_weight, up_weight, down_weight, norm_gain, q, block)
    width = 3 * block
    top, low = layers - 1, 0

    line = exchange(packed[top], "fsdp", Z_GROUPS)
    line = line.reshape(N_Z * rows, width)
    own_x = lax.dynamic_slice_in_dim(saved_inputs, t * half, half, 1)
    cotangent = lax.dynamic_slice_in_dim(out_cotangent, t * half, half, 0)
    shared = share_tokens(jnp.stack([own_x[top], cotangent.astype(BF16), own_x[low]]), line)
    moved = {s: shift_y(line, s) for s in Y_STEPS}
    low_packed = after(packed[low], line)
    line_low = exchange(low_packed, "fsdp", Z_GROUPS)

    x_top = shared[:, 0].reshape(8 * half, d)
    u_top = shared[:, 1].reshape(8 * half, d)
    scale_top = token_scale(x_top)
    line_low = jnp.broadcast_to(line_low.reshape(1, N_Z * rows, width), (N_Y, N_Z * rows, width))
    moved = after(moved, u_top, scale_top, line_low)
    full_top = place(y, [line] + [moved[s] for s in range(1, N_Y)]).reshape(d, width)

    full_low = exchange(line_low, "fsdp", Y_GROUPS).reshape(d, width)
    cols = (((1,), (1,)), ((), ()))
    pick = (lax.broadcasted_iota(jnp.int32, (8, block), 1) == q).astype(BF16)

    def forward(x, u, w, scale):
        gate_w, up_w, down_w = w[:, :block], w[:, block : 2 * block], w[:, 2 * block :]
        gain = lax.dot_general(pick, gate_w, cols, preferred_element_type=F32)[0]
        white = x.astype(F32) * scale
        normed = (white * gain).astype(BF16)
        gate_pre = jnp.dot(normed, gate_w, preferred_element_type=F32)
        up_pre = jnp.dot(normed, up_w, preferred_element_type=F32)
        sig = jax.nn.sigmoid(gate_pre)
        active = gate_pre * sig
        hidden = (active * up_pre).astype(BF16)
        grad_hidden = jnp.dot(u, down_w, preferred_element_type=F32)
        grad_gate = (grad_hidden * up_pre * (sig * (1.0 + gate_pre * (1.0 - sig)))).astype(BF16)
        grad_up = (grad_hidden * active).astype(BF16)
        return gain, white, normed, hidden, grad_gate, grad_up

    def to_normed(grad_gate, grad_up, w):
        partial = lax.dot_general(grad_gate, w[:, :block], cols, preferred_element_type=F32)
        return partial + lax.dot_general(grad_up, w[:, block : 2 * block], cols, preferred_element_type=F32)

    def gain_columns(partial, white):
        gain_part = jnp.sum(partial * white, axis=0)
        gain_high = gain_part.astype(BF16).astype(F32)
        lane = lax.broadcasted_iota(jnp.int32, (d, 128), 1) - (q - block + 128)
        return jnp.where(lane == 0, gain_high[:, None], jnp.where(lane == 1, (gain_part - gain_high)[:, None], 0.0))

    def step_back(cotangent, own_x, grad_normed, gain):
        own = own_x.astype(F32)
        own_scale = lax.rsqrt(jnp.mean(own * own, axis=1, keepdims=True) + epsilon)
        own_white = own * own_scale
        grad_white = grad_normed * gain
        inner = jnp.mean(grad_white * own_white, axis=1, keepdims=True)
        return cotangent + own_scale * (grad_white - own_white * inner)

    gain, white, normed, hidden, gg, gu = forward(x_top, u_top, full_top, scale_top)
    partial = to_normed(gg, gu, full_top).reshape(8, half, d)
    mine = partial[:4] + swap_tp(partial[4:])
    moved = {s: shift_rep(mine[s], -s) for s in REP_STEPS}
    extra = gain_columns(partial.reshape(8 * half, d), white)
    (grads_top,) = weight_grads(after(normed, mine), u_top, gg, gu, hidden, extra)
    received = exchange(grads_top.reshape(N_Y, N_Z * rows, width), "fsdp", Y_GROUPS)
    grad_normed = mine[0]
    for s in REP_STEPS:
        grad_normed = grad_normed + moved[s]
    cotangent = step_back(cotangent, own_x[top], grad_normed, gain)

    x_low = shared[:, 2].reshape(8 * half, d)
    u_low = share_tokens(cotangent.astype(BF16)).reshape(8 * half, d)
    full_low, x_low = after((full_low, x_low), grads_top)
    gain, white, normed, hidden, gg, gu = forward(x_low, u_low, full_low, token_scale(x_low))
    partial = to_normed(gg, gu, full_low).reshape(8, half, d)
    extra = gain_columns(partial.reshape(8 * half, d), white)
    grads_low = weight_grads(normed, u_low, gg, gu, hidden, extra, y)
    moved_y = {s: shift_y(grads_low[s], s) for s in Y_STEPS}

    partial = after(partial, grads_low)
    mine = partial[:4] + swap_tp(partial[4:])
    moved = {s: shift_rep(mine[s], -s) for s in REP_STEPS}
    grad_normed = mine[0]
    for s in REP_STEPS:
        grad_normed = grad_normed + moved[s]
    cotangent = step_back(cotangent, own_x[low], grad_normed, gain)

    received = after(received, grads_low)
    shard_in = sum_narrow([received], q + 2).reshape(N_Z, rows, width)
    shard_top = exchange(shard_in, "fsdp", Z_GROUPS)
    moved_y = after(moved_y, shard_in, mine)
    shard_in = sum_narrow([grads_low[0]] + [moved_y[s] for s in Y_STEPS], q + 2).reshape(N_Z, rows, width)
    shard_low = exchange(shard_in, "fsdp", Z_GROUPS)
    own = jnp.stack([narrow(jnp.sum(widen(v, q + 2), axis=0), q + 2) for v in (shard_low, shard_top)])
    moved = {s: shift_rep(own, s) for s in REP_STEPS}
    pieces = [widen(own, q + 2)] + [widen(moved[s], q + 2) for s in range(1, N_REP)]
    outs = finish(r, pieces, (gate_accum, up_accum, down_accum), q, block)
    gain_sum = sum(jnp.sum(b[:, :, q : q + 2], axis=2) for b in pieces)
    gain_grad = gain_accum + gain_sum + swap_tp(gain_sum)

    other = swap_tp(cotangent)
    both = jnp.stack([cotangent, other])
    cot_out = jnp.concatenate([lax.dynamic_index_in_dim(both, t, 0, False),
                               lax.dynamic_index_in_dim(both, 1 - t, 0, False)], axis=0)
    return (cot_out, outs[0], outs[1], outs[2], gain_grad)


def solution(mesh):
    return jax.shard_map(
        body,
        mesh=mesh,
        in_specs=(
            P(None, ("rep", "fsdp"), None),
            P(("rep", "fsdp"), None),
            P(None, "fsdp", "tp"),
            P(None, "fsdp", "tp"),
            P(None, "fsdp", "tp"),
            P(None, "fsdp"),
            P(None, "fsdp", "tp"),
            P(None, "fsdp", "tp"),
            P(None, "fsdp", "tp"),
            P(None, "fsdp"),
        ),
        out_specs=(
            P(("rep", "fsdp"), None),
            P(None, "fsdp", "tp"),
            P(None, "fsdp", "tp"),
            P(None, "fsdp", "tp"),
            P(None, "fsdp"),
        ),
        check_vma=False,
    )
```

```python
import functools

import jax
import jax.numpy as jnp
from jax import lax
from jax.experimental import pallas as pl
from jax.experimental.pallas import tpu as pltpu
from jax.sharding import PartitionSpec as P

epsilon = 1e-06
F32, BF16, F16 = jnp.float32, jnp.bfloat16, jnp.float16


N_Y, N_Z, N_REP = 4, 8, 4
REP_STEPS = (1, 3, 2)
Y_STEPS = (1, 3, 2)
VMEM = pl.BlockSpec(memory_space=pltpu.VMEM)
SMEM = pl.BlockSpec(memory_space=pltpu.SMEM)


def shift_rep(value, step):
    return lax.ppermute(value, "rep", [(i, (i + step) % N_REP) for i in range(N_REP)])


def swap_tp(value):
    return lax.ppermute(value, "tp", [(0, 1), (1, 0)])


def shift_y(value, step):
    pairs = [(y * N_Z + z, (y + step) % N_Y * N_Z + z) for y in range(N_Y) for z in range(N_Z)]
    return lax.ppermute(value, "fsdp", pairs)


Y_GROUPS = [[y * N_Z + z for y in range(N_Y)] for z in range(N_Z)]
Z_GROUPS = [[y * N_Z + z for z in range(N_Z)] for y in range(N_Y)]


def exchange(value, axis, groups=None):
    return lax.all_to_all(value, axis, 0, 0, tiled=True, axis_index_groups=groups)


def after(value, *others):
    return lax.optimization_barrier((value, others))[0]


def pack_kernel(q, block, r_ref, gate_ref, up_ref, down_ref, gain_ref, *refs):
    outs, one = refs[:-1], refs[-1]
    rows = gate_ref.shape[1]
    row = lax.broadcasted_iota(jnp.int32, (rows, rows), 0)
    diagonal = row == lax.broadcasted_iota(jnp.int32, (rows, rows), 1)
    for l, out in enumerate(outs):
        gain = jnp.where(diagonal, gain_ref[l : l + 1].astype(F32), 0.0)
        one[...] = jnp.zeros_like(one)
        one[:, q : q + 1] = jnp.sum(gain, axis=1, keepdims=True).astype(BF16)
        for k in range(N_REP):

            @pl.when(r_ref[0] == k)
            def _():
                for i, w in enumerate((gate_ref, up_ref, down_ref)):
                    one[:, i * block : i * block + q] = w[l, :, k * q : (k + 1) * q]

        for i in range(N_Z):
            out[i] = one[...]


def pack(r, gate, up, down, gain, q, block):
    layers, rows, _ = gate.shape
    return pl.pallas_call(
        functools.partial(pack_kernel, q, block),
        out_shape=[jax.ShapeDtypeStruct((N_Z, rows, 3 * block), BF16)] * layers,
        in_specs=[SMEM] + [VMEM] * 4,
        out_specs=[VMEM] * layers,
        scratch_shapes=[pltpu.VMEM((rows, 3 * block), BF16)],
        cost_estimate=pl.CostEstimate(flops=1000000, bytes_accessed=1000000, transcendentals=0),
        name="pack",
    )(r.reshape(1), gate, up, down, gain)


def place_kernel(n, me_ref, *refs):
    out_ref = refs[n]
    for s in range(n):
        out_ref[lax.rem(me_ref[0] + (n - s), n)] = refs[s][...]


def place(me, pieces):
    n = len(pieces)
    return pl.pallas_call(
        functools.partial(place_kernel, n),
        out_shape=jax.ShapeDtypeStruct((n,) + pieces[0].shape, pieces[0].dtype),
        in_specs=[SMEM] + [VMEM] * n,
        out_specs=VMEM,
        cost_estimate=pl.CostEstimate(flops=1000000, bytes_accessed=2 * n * pieces[0].size * 2, transcendentals=0),
        name="place",
    )(me.reshape(1), *pieces)


def share_tokens(own, *others):
    moved = {s: shift_rep(own, s) for s in REP_STEPS}
    if others:
        moved = after(moved, *others)
    mine = jnp.stack([own] + [moved[s] for s in range(1, N_REP)])
    swapped = swap_tp(mine)
    return jnp.concatenate([mine, swapped], axis=0)


def products(block, normed_ref, u_ref, gg_ref, gu_ref, hid_ref, extra_ref, write):
    contract = (((0,), (0,)), ((), ()))
    for i, (left, right) in enumerate(((normed_ref, gg_ref), (normed_ref, gu_ref), (u_ref, hid_ref))):
        product = lax.dot_general(left[...], right[...], contract, preferred_element_type=F32)
        if i == 0:
            write(0, block - 128, product[:, : block - 128])
            write(block - 128, block, product[:, block - 128 :] + extra_ref[...])
        else:
            write(i * block, (i + 1) * block, product)


def grads_kernel(block, *refs):
    def write(start, stop, value):
        refs[6][:, start:stop] = value.astype(BF16)

    products(block, *refs[:6], write)


def grads_blocks_kernel(rows, block, y_ref, *refs):
    outs, acc = refs[6:10], refs[10]

    def write(start, stop, value):
        acc[:, : stop - start] = value
        for s in range(N_Y):
            first = pl.multiple_of(lax.rem(y_ref[0] + s, N_Y) * rows, rows)
            outs[s][:, start:stop] = acc[pl.ds(first, rows), : stop - start].astype(outs[s].dtype)

    products(block, *refs[:6], write)


def weight_grads(normed, u, gg, gu, hid, extra, y=None):
    tokens, d = normed.shape
    block = gg.shape[1]
    rows = d // N_Y
    if y is None:
        shapes, kernel, scratch, first = [(d, BF16)], functools.partial(grads_kernel, block), [], ()
    else:
        shapes, kernel = [(rows, F32)] + [(rows, BF16)] * 3, functools.partial(grads_blocks_kernel, rows, block)
        scratch, first = [pltpu.VMEM((d, block), F32)], (y.reshape(1),)
    return pl.pallas_call(
        kernel,
        out_shape=[jax.ShapeDtypeStruct((n, 3 * block), dtype) for n, dtype in shapes],
        in_specs=[SMEM] * len(first) + [VMEM] * 6,
        out_specs=[VMEM] * len(shapes),
        scratch_shapes=scratch,
        cost_estimate=pl.CostEstimate(flops=6 * tokens * d * block, bytes_accessed=10000000, transcendentals=0),
        compiler_params=pltpu.CompilerParams(vmem_limit_bytes=48 * 1024 * 1024),
        name="weight_grads",
    )(*first, normed, u, gg, gu, hid, extra)


def narrow(value, lane):
    most = jnp.max(jnp.abs(value), axis=-1, keepdims=True)
    e = jnp.where(most > 0.0, jnp.clip(jnp.ceil(jnp.log2(most)) - 12.0, -120.0, 120.0), 0.0)
    lanes = lax.broadcasted_iota(jnp.int32, value.shape, value.ndim - 1)
    return jnp.where(lanes == lane, e, value * jnp.exp2(-e)).astype(F16)


def widen(value, lane):
    return value.astype(F32) * jnp.exp2(value[..., lane : lane + 1].astype(F32))


def finish_kernel(q, block, layers, r_ref, b0, b1, b2, b3, *refs):
    accums, outs, stack = refs[:3], refs[3:6], refs[6]
    for s, b in enumerate((b0, b1, b2, b3)):
        stack[lax.rem(r_ref[0] + (N_REP - s), N_REP)] = b[...]
    for l in range(layers):
        for i in range(3):
            whole = jnp.concatenate([stack[k, l, :, i * block : i * block + q] for k in range(N_REP)], axis=1)
            outs[i][l] = accums[i][l] + whole


def finish(r, pieces, accums, q, block):
    return pl.pallas_call(
        functools.partial(finish_kernel, q, block, accums[0].shape[0]),
        out_shape=[jax.ShapeDtypeStruct(accums[0].shape, F32)] * 3,
        in_specs=[SMEM] + [VMEM] * 7,
        out_specs=[VMEM] * 3,
        scratch_shapes=[pltpu.VMEM((N_REP,) + pieces[0].shape, F32)],
        cost_estimate=pl.CostEstimate(flops=1000000, bytes_accessed=2000000, transcendentals=0),
        name="finish",
    )(r.reshape(1), *pieces, *accums)


def token_scale(x):
    x = x.astype(F32)
    return lax.rsqrt(jnp.mean(x * x, axis=1, keepdims=True) + epsilon)


def body(
    saved_inputs,
    out_cotangent,
    gate_weight,
    up_weight,
    down_weight,
    norm_gain,
    gate_accum,
    up_accum,
    down_accum,
    gain_accum,
):
    layers, tokens, d = saved_inputs.shape
    rows, hidden_local = gate_weight.shape[1:]
    q = hidden_local // N_REP
    block = -(-(q + 2) // 128) * 128
    half = tokens // 2
    r, f, t = lax.axis_index("rep"), lax.axis_index("fsdp"), lax.axis_index("tp")
    y = f // N_Z

    packed = pack(r, gate_weight, up_weight, down_weight, norm_gain, q, block)
    width = 3 * block
    top, low = layers - 1, 0

    line = exchange(packed[top], "fsdp", Z_GROUPS)
    line = line.reshape(N_Z * rows, width)
    own_x = lax.dynamic_slice_in_dim(saved_inputs, t * half, half, 1)
    cotangent = lax.dynamic_slice_in_dim(out_cotangent, t * half, half, 0)
    shared = share_tokens(jnp.stack([own_x[top], cotangent.astype(BF16), own_x[low]]), line)
    moved = {s: shift_y(line, s) for s in Y_STEPS}
    x_top = shared[:, 0].reshape(8 * half, d)
    u_top = shared[:, 1].reshape(8 * half, d)
    scale_top = token_scale(x_top)
    moved = after(moved, u_top, scale_top)
    full_top = place(y, [line] + [moved[s] for s in range(1, N_Y)]).reshape(d, width)

    low_packed = after(packed[low], line)
    line = exchange(low_packed, "fsdp", Z_GROUPS)
    line_low = line.reshape(N_Z * rows, width)
    cols = (((1,), (1,)), ((), ()))
    pick = (lax.broadcasted_iota(jnp.int32, (8, block), 1) == q).astype(BF16)

    def forward(x, u, w, scale):
        gate_w, up_w, down_w = w[:, :block], w[:, block : 2 * block], w[:, 2 * block :]
        gain = lax.dot_general(pick, gate_w, cols, preferred_element_type=F32)[0]
        white = x.astype(F32) * scale
        normed = (white * gain).astype(BF16)
        gate_pre = jnp.dot(normed, gate_w, preferred_element_type=F32)
        up_pre = jnp.dot(normed, up_w, preferred_element_type=F32)
        sig = jax.nn.sigmoid(gate_pre)
        active = gate_pre * sig
        hidden = (active * up_pre).astype(BF16)
        grad_hidden = jnp.dot(u, down_w, preferred_element_type=F32)
        grad_gate = (grad_hidden * up_pre * (sig * (1.0 + gate_pre * (1.0 - sig)))).astype(BF16)
        grad_up = (grad_hidden * active).astype(BF16)
        return gain, white, normed, hidden, grad_gate, grad_up

    def to_normed(grad_gate, grad_up, w):
        partial = lax.dot_general(grad_gate, w[:, :block], cols, preferred_element_type=F32)
        return partial + lax.dot_general(grad_up, w[:, block : 2 * block], cols, preferred_element_type=F32)

    def gain_columns(partial, white):
        gain_part = jnp.sum(partial * white, axis=0)
        gain_high = gain_part.astype(BF16).astype(F32)
        lane = lax.broadcasted_iota(jnp.int32, (d, 128), 1) - (q - block + 128)
        return jnp.where(lane == 0, gain_high[:, None], jnp.where(lane == 1, (gain_part - gain_high)[:, None], 0.0))

    def step_back(cotangent, own_x, grad_normed, gain):
        own = own_x.astype(F32)
        own_scale = lax.rsqrt(jnp.mean(own * own, axis=1, keepdims=True) + epsilon)
        own_white = own * own_scale
        grad_white = grad_normed * gain
        inner = jnp.mean(grad_white * own_white, axis=1, keepdims=True)
        return cotangent + own_scale * (grad_white - own_white * inner)

    gain, white, normed, hidden, gg, gu = forward(x_top, u_top, full_top, scale_top)
    partial = to_normed(gg, gu, full_top).reshape(8, half, d)
    mine = partial[:4] + swap_tp(partial[4:])
    moved = {s: shift_rep(mine[s], -s) for s in REP_STEPS}
    line_low = after(line_low, mine)
    moved_low = {3: shift_y(line_low, 3)}
    moved_low |= {s: shift_y(line_low, s) for s in (2, 1)}
    extra = gain_columns(partial.reshape(8 * half, d), white)
    (grads_top,) = weight_grads(after(normed, mine), u_top, gg, gu, hidden, extra)
    received = exchange(grads_top.reshape(N_Y, N_Z * rows, width), "fsdp", Y_GROUPS)
    grad_normed = mine[0]
    for s in REP_STEPS:
        grad_normed = grad_normed + moved[s]
    cotangent = step_back(cotangent, own_x[top], grad_normed, gain)

    x_low = shared[:, 2].reshape(8 * half, d)
    u_low = share_tokens(cotangent.astype(BF16)).reshape(8 * half, d)
    moved_low, x_low = after((moved_low, x_low), cotangent, grads_top)
    full_low = place(y, [line_low] + [moved_low[s] for s in range(1, N_Y)]).reshape(d, width)
    gain, white, normed, hidden, gg, gu = forward(x_low, u_low, full_low, token_scale(x_low))
    partial = to_normed(gg, gu, full_low).reshape(8, half, d)
    extra = gain_columns(partial.reshape(8 * half, d), white)
    grads_low = weight_grads(normed, u_low, gg, gu, hidden, extra, y)
    moved_y = {s: shift_y(grads_low[s], s) for s in Y_STEPS}

    partial = after(partial, grads_low)
    mine = partial[:4] + swap_tp(partial[4:])
    moved = {s: shift_rep(mine[s], -s) for s in REP_STEPS}
    grad_normed = mine[0]
    for s in REP_STEPS:
        grad_normed = grad_normed + moved[s]
    cotangent = step_back(cotangent, own_x[low], grad_normed, gain)

    received = after(received, grads_low)
    total = jnp.sum(received.astype(F32), axis=0)
    shard_in = narrow(total, q + 2).reshape(N_Z, rows, width)
    shard_top = exchange(shard_in, "fsdp", Z_GROUPS)
    moved_y = after(moved_y, shard_in, mine)
    total = grads_low[0]
    for s in Y_STEPS:
        total = total + moved_y[s].astype(F32)
    shard_in = narrow(total, q + 2).reshape(N_Z, rows, width)
    shard_low = exchange(shard_in, "fsdp", Z_GROUPS)
    own = jnp.stack([narrow(jnp.sum(widen(v, q + 2), axis=0), q + 2) for v in (shard_low, shard_top)])
    moved = {s: shift_rep(own, s) for s in REP_STEPS}
    pieces = [widen(own, q + 2)] + [widen(moved[s], q + 2) for s in range(1, N_REP)]
    outs = finish(r, pieces, (gate_accum, up_accum, down_accum), q, block)
    gain_sum = sum(jnp.sum(b[:, :, q : q + 2], axis=2) for b in pieces)
    gain_grad = gain_accum + gain_sum + swap_tp(gain_sum)

    other = swap_tp(cotangent)
    both = jnp.stack([cotangent, other])
    cot_out = jnp.concatenate([lax.dynamic_index_in_dim(both, t, 0, False),
                               lax.dynamic_index_in_dim(both, 1 - t, 0, False)], axis=0)
    return (cot_out, outs[0], outs[1], outs[2], gain_grad)


def solution(mesh):
    return jax.shard_map(
        body,
        mesh=mesh,
        in_specs=(
            P(None, ("rep", "fsdp"), None),
            P(("rep", "fsdp"), None),
            P(None, "fsdp", "tp"),
            P(None, "fsdp", "tp"),
            P(None, "fsdp", "tp"),
            P(None, "fsdp"),
            P(None, "fsdp", "tp"),
            P(None, "fsdp", "tp"),
            P(None, "fsdp", "tp"),
            P(None, "fsdp"),
        ),
        out_specs=(
            P(("rep", "fsdp"), None),
            P(None, "fsdp", "tp"),
            P(None, "fsdp", "tp"),
            P(None, "fsdp", "tp"),
            P(None, "fsdp"),
        ),
        check_vma=False,
    )
```

```python
import functools

import jax
import jax.numpy as jnp
from jax import lax
from jax.experimental import pallas as pl
from jax.experimental.pallas import tpu as pltpu
from jax.sharding import PartitionSpec as P

epsilon = 1e-06
F32, BF16, F16 = jnp.float32, jnp.bfloat16, jnp.float16


N_Y, N_Z, N_REP = 4, 8, 4
REP_STEPS = (1, 3, 2)
Y_STEPS = (1, 3, 2)
VMEM = pl.BlockSpec(memory_space=pltpu.VMEM)
SMEM = pl.BlockSpec(memory_space=pltpu.SMEM)


def shift_rep(value, step):
    return lax.ppermute(value, "rep", [(i, (i + step) % N_REP) for i in range(N_REP)])


def swap_tp(value):
    return lax.ppermute(value, "tp", [(0, 1), (1, 0)])


def shift_y(value, step):
    pairs = [(y * N_Z + z, (y + step) % N_Y * N_Z + z) for y in range(N_Y) for z in range(N_Z)]
    return lax.ppermute(value, "fsdp", pairs)


Y_GROUPS = [[y * N_Z + z for y in range(N_Y)] for z in range(N_Z)]
Z_GROUPS = [[y * N_Z + z for z in range(N_Z)] for y in range(N_Y)]


def exchange(value, axis, groups=None):
    return lax.all_to_all(value, axis, 0, 0, tiled=True, axis_index_groups=groups)


def after(value, *others):
    return lax.optimization_barrier((value, others))[0]


def parts_of(width):
    first = -(-width // 256) * 128
    return first, width - first


def pack_kernel(q, block, r_ref, gate_ref, up_ref, down_ref, gain_ref, *refs):
    outs, first, second, one = refs[:-3], *refs[-3:]
    rows = gate_ref.shape[1]
    row = lax.broadcasted_iota(jnp.int32, (rows, rows), 0)
    diagonal = row == lax.broadcasted_iota(jnp.int32, (rows, rows), 1)
    cut = first.shape[-1]
    for l in range(len(outs) + 1):
        gain = jnp.where(diagonal, gain_ref[l : l + 1].astype(F32), 0.0)
        one[...] = jnp.zeros_like(one)
        one[:, q : q + 1] = jnp.sum(gain, axis=1, keepdims=True).astype(BF16)
        for k in range(N_REP):

            @pl.when(r_ref[0] == k)
            def _():
                for i, w in enumerate((gate_ref, up_ref, down_ref)):
                    one[:, i * block : i * block + q] = w[l, :, k * q : (k + 1) * q]

        for i in range(N_Z):
            if l < len(outs):
                outs[l][i] = one[...]
            else:
                first[i] = one[:, :cut]
                second[i] = one[:, cut:]


def pack(r, gate, up, down, gain, q, block):
    layers, rows, _ = gate.shape
    return pl.pallas_call(
        functools.partial(pack_kernel, q, block),
        out_shape=[jax.ShapeDtypeStruct((N_Z, rows, 3 * block), BF16)] * (layers - 1)
        + [jax.ShapeDtypeStruct((N_Z, rows, n), BF16) for n in parts_of(3 * block)],
        in_specs=[SMEM] + [VMEM] * 4,
        out_specs=[VMEM] * (layers + 1),
        scratch_shapes=[pltpu.VMEM((rows, 3 * block), BF16)],
        cost_estimate=pl.CostEstimate(flops=1000000, bytes_accessed=1000000, transcendentals=0),
        name="pack",
    )(r.reshape(1), gate, up, down, gain)


def place_kernel(n, parts, me_ref, *refs):
    out_ref = refs[-1]
    for s in range(n):
        start = 0
        for p in range(parts):
            piece = refs[p * n + s]
            out_ref[lax.rem(me_ref[0] + (n - s), n), :, start : start + piece.shape[1]] = piece[...]
            start += piece.shape[1]


def place(me, *parts):
    n = len(parts[0])
    pieces = [piece for part in parts for piece in part]
    rows, width = pieces[0].shape[0], sum(part[0].shape[1] for part in parts)
    return pl.pallas_call(
        functools.partial(place_kernel, n, len(parts)),
        out_shape=jax.ShapeDtypeStruct((n, rows, width), pieces[0].dtype),
        in_specs=[SMEM] + [VMEM] * len(pieces),
        out_specs=VMEM,
        cost_estimate=pl.CostEstimate(flops=1000000, bytes_accessed=4 * n * rows * width, transcendentals=0),
        name="place",
    )(me.reshape(1), *pieces)


def share_tokens(own, *others):
    moved = {s: shift_rep(own, s) for s in REP_STEPS}
    if others:
        moved = after(moved, *others)
    mine = jnp.stack([own] + [moved[s] for s in range(1, N_REP)])
    swapped = swap_tp(mine)
    return jnp.concatenate([mine, swapped], axis=0)


def products(block, normed_ref, u_ref, gg_ref, gu_ref, hid_ref, extra_ref, write):
    contract = (((0,), (0,)), ((), ()))
    for i, (left, right) in enumerate(((normed_ref, gg_ref), (normed_ref, gu_ref), (u_ref, hid_ref))):
        product = lax.dot_general(left[...], right[...], contract, preferred_element_type=F32)
        if i == 0:
            write(0, block - 128, product[:, : block - 128])
            write(block - 128, block, product[:, block - 128 :] + extra_ref[...])
        else:
            write(i * block, (i + 1) * block, product)


def grads_kernel(block, *refs):
    def write(start, stop, value):
        refs[6][:, start:stop] = value.astype(BF16)

    products(block, *refs[:6], write)


def grads_blocks_kernel(rows, block, y_ref, *refs):
    outs, acc = refs[6:10], refs[10]

    def write(start, stop, value):
        acc[:, : stop - start] = value
        for s in range(N_Y):
            first = pl.multiple_of(lax.rem(y_ref[0] + s, N_Y) * rows, rows)
            outs[s][:, start:stop] = acc[pl.ds(first, rows), : stop - start].astype(outs[s].dtype)

    products(block, *refs[:6], write)


def weight_grads(normed, u, gg, gu, hid, extra, y=None):
    tokens, d = normed.shape
    block = gg.shape[1]
    rows = d // N_Y
    if y is None:
        shapes, kernel, scratch, first = [(d, BF16)], functools.partial(grads_kernel, block), [], ()
    else:
        shapes, kernel = [(rows, F32)] + [(rows, BF16)] * 3, functools.partial(grads_blocks_kernel, rows, block)
        scratch, first = [pltpu.VMEM((d, block), F32)], (y.reshape(1),)
    return pl.pallas_call(
        kernel,
        out_shape=[jax.ShapeDtypeStruct((n, 3 * block), dtype) for n, dtype in shapes],
        in_specs=[SMEM] * len(first) + [VMEM] * 6,
        out_specs=[VMEM] * len(shapes),
        scratch_shapes=scratch,
        cost_estimate=pl.CostEstimate(flops=6 * tokens * d * block, bytes_accessed=10000000, transcendentals=0),
        compiler_params=pltpu.CompilerParams(vmem_limit_bytes=48 * 1024 * 1024),
        name="weight_grads",
    )(*first, normed, u, gg, gu, hid, extra)


def narrow(value, lane):
    most = jnp.max(jnp.abs(value), axis=-1, keepdims=True)
    e = jnp.where(most > 0.0, jnp.clip(jnp.ceil(jnp.log2(most)) - 12.0, -120.0, 120.0), 0.0)
    lanes = lax.broadcasted_iota(jnp.int32, value.shape, value.ndim - 1)
    return jnp.where(lanes == lane, e, value * jnp.exp2(-e)).astype(F16)


def widen(value, lane):
    return value.astype(F32) * jnp.exp2(value[..., lane : lane + 1].astype(F32))


def finish_kernel(q, block, layers, r_ref, b0, b1, b2, b3, *refs):
    accums, outs, stack = refs[:3], refs[3:6], refs[6]
    for s, b in enumerate((b0, b1, b2, b3)):
        stack[lax.rem(r_ref[0] + (N_REP - s), N_REP)] = b[...]
    for l in range(layers):
        for i in range(3):
            whole = jnp.concatenate([stack[k, l, :, i * block : i * block + q] for k in range(N_REP)], axis=1)
            outs[i][l] = accums[i][l] + whole


def finish(r, pieces, accums, q, block):
    return pl.pallas_call(
        functools.partial(finish_kernel, q, block, accums[0].shape[0]),
        out_shape=[jax.ShapeDtypeStruct(accums[0].shape, F32)] * 3,
        in_specs=[SMEM] + [VMEM] * 7,
        out_specs=[VMEM] * 3,
        scratch_shapes=[pltpu.VMEM((N_REP,) + pieces[0].shape, F32)],
        cost_estimate=pl.CostEstimate(flops=1000000, bytes_accessed=2000000, transcendentals=0),
        name="finish",
    )(r.reshape(1), *pieces, *accums)


def token_scale(x):
    x = x.astype(F32)
    return lax.rsqrt(jnp.mean(x * x, axis=1, keepdims=True) + epsilon)


def body(
    saved_inputs,
    out_cotangent,
    gate_weight,
    up_weight,
    down_weight,
    norm_gain,
    gate_accum,
    up_accum,
    down_accum,
    gain_accum,
):
    layers, tokens, d = saved_inputs.shape
    rows, hidden_local = gate_weight.shape[1:]
    q = hidden_local // N_REP
    block = -(-(q + 2) // 128) * 128
    half = tokens // 2
    r, f, t = lax.axis_index("rep"), lax.axis_index("fsdp"), lax.axis_index("tp")
    y = f // N_Z

    packed = pack(r, gate_weight, up_weight, down_weight, norm_gain, q, block)
    width = 3 * block
    top, low = layers - 1, 0

    lines = []
    for part in packed[top:]:
        lines.append(exchange(part, "fsdp", Z_GROUPS).reshape(N_Z * rows, part.shape[2]))
    line = lines[-1]
    own_x = lax.dynamic_slice_in_dim(saved_inputs, t * half, half, 1)
    cotangent = lax.dynamic_slice_in_dim(out_cotangent, t * half, half, 0)
    shared = share_tokens(jnp.stack([own_x[top], cotangent.astype(BF16), own_x[low]]), line)
    moved = []
    for part in lines:
        moved.append({s: shift_y(part, s) for s in Y_STEPS})
    x_top = shared[:, 0].reshape(8 * half, d)
    u_top = shared[:, 1].reshape(8 * half, d)
    scale_top = token_scale(x_top)
    moved = after(moved, u_top, scale_top)
    full_top = place(y, *([part] + [m[s] for s in range(1, N_Y)] for part, m in zip(lines, moved))).reshape(d, width)

    low_packed = after(packed[low], line)
    line = exchange(low_packed, "fsdp", Z_GROUPS)
    line_low = line.reshape(N_Z * rows, width)
    cols = (((1,), (1,)), ((), ()))
    pick = (lax.broadcasted_iota(jnp.int32, (8, block), 1) == q).astype(BF16)

    def forward(x, u, w, scale):
        gate_w, up_w, down_w = w[:, :block], w[:, block : 2 * block], w[:, 2 * block :]
        gain = lax.dot_general(pick, gate_w, cols, preferred_element_type=F32)[0]
        white = x.astype(F32) * scale
        normed = (white * gain).astype(BF16)
        gate_pre = jnp.dot(normed, gate_w, preferred_element_type=F32)
        up_pre = jnp.dot(normed, up_w, preferred_element_type=F32)
        sig = jax.nn.sigmoid(gate_pre)
        active = gate_pre * sig
        hidden = (active * up_pre).astype(BF16)
        grad_hidden = jnp.dot(u, down_w, preferred_element_type=F32)
        grad_gate = (grad_hidden * up_pre * (sig * (1.0 + gate_pre * (1.0 - sig)))).astype(BF16)
        grad_up = (grad_hidden * active).astype(BF16)
        return gain, white, normed, hidden, grad_gate, grad_up

    def to_normed(grad_gate, grad_up, w):
        partial = lax.dot_general(grad_gate, w[:, :block], cols, preferred_element_type=F32)
        return partial + lax.dot_general(grad_up, w[:, block : 2 * block], cols, preferred_element_type=F32)

    def gain_columns(partial, white):
        gain_part = jnp.sum(partial * white, axis=0)
        gain_high = gain_part.astype(BF16).astype(F32)
        lane = lax.broadcasted_iota(jnp.int32, (d, 128), 1) - (q - block + 128)
        return jnp.where(lane == 0, gain_high[:, None], jnp.where(lane == 1, (gain_part - gain_high)[:, None], 0.0))

    def step_back(cotangent, own_x, grad_normed, gain):
        own = own_x.astype(F32)
        own_scale = lax.rsqrt(jnp.mean(own * own, axis=1, keepdims=True) + epsilon)
        own_white = own * own_scale
        grad_white = grad_normed * gain
        inner = jnp.mean(grad_white * own_white, axis=1, keepdims=True)
        return cotangent + own_scale * (grad_white - own_white * inner)

    gain, white, normed, hidden, gg, gu = forward(x_top, u_top, full_top, scale_top)
    partial = to_normed(gg, gu, full_top).reshape(8, half, d)
    mine = partial[:4] + swap_tp(partial[4:])
    moved = {s: shift_rep(mine[s], -s) for s in REP_STEPS}
    line_low = after(line_low, mine)
    moved_low = {2: shift_y(line_low, 2)}
    moved_low |= {s: shift_y(line_low, s) for s in (1, 3)}
    extra = gain_columns(partial.reshape(8 * half, d), white)
    (grads_top,) = weight_grads(after(normed, mine), u_top, gg, gu, hidden, extra)
    received = exchange(grads_top.reshape(N_Y, N_Z * rows, width), "fsdp", Y_GROUPS)
    grad_normed = mine[0]
    for s in REP_STEPS:
        grad_normed = grad_normed + moved[s]
    cotangent = step_back(cotangent, own_x[top], grad_normed, gain)

    x_low = shared[:, 2].reshape(8 * half, d)
    u_low = share_tokens(cotangent.astype(BF16)).reshape(8 * half, d)
    moved_low, x_low = after((moved_low, x_low), cotangent, grads_top)
    full_low = place(y, [line_low] + [moved_low[s] for s in range(1, N_Y)]).reshape(d, width)
    gain, white, normed, hidden, gg, gu = forward(x_low, u_low, full_low, token_scale(x_low))
    partial = to_normed(gg, gu, full_low).reshape(8, half, d)
    extra = gain_columns(partial.reshape(8 * half, d), white)
    grads_low = weight_grads(normed, u_low, gg, gu, hidden, extra, y)
    moved_y = {s: shift_y(grads_low[s], s) for s in Y_STEPS}

    partial = after(partial, grads_low)
    mine = partial[:4] + swap_tp(partial[4:])
    moved = {s: shift_rep(mine[s], -s) for s in REP_STEPS}
    grad_normed = mine[0]
    for s in REP_STEPS:
        grad_normed = grad_normed + moved[s]
    cotangent = step_back(cotangent, own_x[low], grad_normed, gain)

    received = after(received, grads_low)
    total = jnp.sum(received.astype(F32), axis=0)
    shard_in = narrow(total, q + 2).reshape(N_Z, rows, width)
    shard_top = exchange(shard_in, "fsdp", Z_GROUPS)
    moved_y = after(moved_y, shard_in, mine)
    total = grads_low[0]
    for s in Y_STEPS:
        total = total + moved_y[s].astype(F32)
    shard_in = narrow(total, q + 2).reshape(N_Z, rows, width)
    shard_low = exchange(shard_in, "fsdp", Z_GROUPS)
    own = jnp.stack([narrow(jnp.sum(widen(v, q + 2), axis=0), q + 2) for v in (shard_low, shard_top)])
    moved = {s: shift_rep(own, s) for s in REP_STEPS}
    pieces = [widen(own, q + 2)] + [widen(moved[s], q + 2) for s in range(1, N_REP)]
    outs = finish(r, pieces, (gate_accum, up_accum, down_accum), q, block)
    gain_sum = sum(jnp.sum(b[:, :, q : q + 2], axis=2) for b in pieces)
    gain_grad = gain_accum + gain_sum + swap_tp(gain_sum)

    other = swap_tp(cotangent)
    both = jnp.stack([cotangent, other])
    cot_out = jnp.concatenate([lax.dynamic_index_in_dim(both, t, 0, False),
                               lax.dynamic_index_in_dim(both, 1 - t, 0, False)], axis=0)
    return (cot_out, outs[0], outs[1], outs[2], gain_grad)


def solution(mesh):
    return jax.shard_map(
        body,
        mesh=mesh,
        in_specs=(
            P(None, ("rep", "fsdp"), None),
            P(("rep", "fsdp"), None),
            P(None, "fsdp", "tp"),
            P(None, "fsdp", "tp"),
            P(None, "fsdp", "tp"),
            P(None, "fsdp"),
            P(None, "fsdp", "tp"),
            P(None, "fsdp", "tp"),
            P(None, "fsdp", "tp"),
            P(None, "fsdp"),
        ),
        out_specs=(
            P(("rep", "fsdp"), None),
            P(None, "fsdp", "tp"),
            P(None, "fsdp", "tp"),
            P(None, "fsdp", "tp"),
            P(None, "fsdp"),
        ),
        check_vma=False,
    )
```

```python
import functools

import jax
import jax.numpy as jnp
from jax import lax
from jax.experimental import pallas as pl
from jax.experimental.pallas import tpu as pltpu
from jax.sharding import PartitionSpec as P

epsilon = 1e-06
F32, BF16, F16 = jnp.float32, jnp.bfloat16, jnp.float16


N_Y, N_Z, N_REP = 4, 8, 4
REP_STEPS = (1, 3, 2)
Y_STEPS = (1, 3, 2)
VMEM = pl.BlockSpec(memory_space=pltpu.VMEM)
SMEM = pl.BlockSpec(memory_space=pltpu.SMEM)


def shift_rep(value, step):
    return lax.ppermute(value, "rep", [(i, (i + step) % N_REP) for i in range(N_REP)])


def swap_tp(value):
    return lax.ppermute(value, "tp", [(0, 1), (1, 0)])


def shift_y(value, step):
    pairs = [(y * N_Z + z, (y + step) % N_Y * N_Z + z) for y in range(N_Y) for z in range(N_Z)]
    return lax.ppermute(value, "fsdp", pairs)


Y_GROUPS = [[y * N_Z + z for y in range(N_Y)] for z in range(N_Z)]
Z_GROUPS = [[y * N_Z + z for z in range(N_Z)] for y in range(N_Y)]


def exchange(value, axis, groups=None):
    return lax.all_to_all(value, axis, 0, 0, tiled=True, axis_index_groups=groups)


def after(value, *others):
    return lax.optimization_barrier((value, others))[0]


def parts_of(width):
    first = -(-width // 256) * 128
    return first, width - first


def pack_kernel(q, block, r_ref, gate_ref, up_ref, down_ref, gain_ref, *refs):
    outs, first, second, one = refs[:-3], *refs[-3:]
    rows = gate_ref.shape[1]
    row = lax.broadcasted_iota(jnp.int32, (rows, rows), 0)
    diagonal = row == lax.broadcasted_iota(jnp.int32, (rows, rows), 1)
    cut = first.shape[-1]
    for l in range(len(outs) + 1):
        gain = jnp.where(diagonal, gain_ref[l : l + 1].astype(F32), 0.0)
        one[...] = jnp.zeros_like(one)
        one[:, q : q + 1] = jnp.sum(gain, axis=1, keepdims=True).astype(BF16)
        for k in range(N_REP):

            @pl.when(r_ref[0] == k)
            def _():
                for i, w in enumerate((gate_ref, up_ref, down_ref)):
                    one[:, i * block : i * block + q] = w[l, :, k * q : (k + 1) * q]

        for i in range(N_Z):
            if l < len(outs):
                outs[l][i] = one[...]
            else:
                first[i] = one[:, :cut]
                second[i] = one[:, cut:]


def pack(r, gate, up, down, gain, q, block):
    layers, rows, _ = gate.shape
    return pl.pallas_call(
        functools.partial(pack_kernel, q, block),
        out_shape=[jax.ShapeDtypeStruct((N_Z, rows, 3 * block), BF16)] * (layers - 1)
        + [jax.ShapeDtypeStruct((N_Z, rows, n), BF16) for n in parts_of(3 * block)],
        in_specs=[SMEM] + [VMEM] * 4,
        out_specs=[VMEM] * (layers + 1),
        scratch_shapes=[pltpu.VMEM((rows, 3 * block), BF16)],
        cost_estimate=pl.CostEstimate(flops=1000000, bytes_accessed=1000000, transcendentals=0),
        name="pack",
    )(r.reshape(1), gate, up, down, gain)


def place_kernel(n, parts, me_ref, *refs):
    out_ref = refs[-1]
    for s in range(n):
        start = 0
        for p in range(parts):
            piece = refs[p * n + s]
            out_ref[lax.rem(me_ref[0] + (n - s), n), :, start : start + piece.shape[1]] = piece[...]
            start += piece.shape[1]


def place(me, *parts):
    n = len(parts[0])
    pieces = [piece for part in parts for piece in part]
    rows, width = pieces[0].shape[0], sum(part[0].shape[1] for part in parts)
    return pl.pallas_call(
        functools.partial(place_kernel, n, len(parts)),
        out_shape=jax.ShapeDtypeStruct((n, rows, width), pieces[0].dtype),
        in_specs=[SMEM] + [VMEM] * len(pieces),
        out_specs=VMEM,
        cost_estimate=pl.CostEstimate(flops=1000000, bytes_accessed=4 * n * rows * width, transcendentals=0),
        name="place",
    )(me.reshape(1), *pieces)


def share_tokens(own, *others):
    moved = {s: shift_rep(own, s) for s in REP_STEPS}
    if others:
        moved, own = after((moved, own), *others)
    mine = jnp.stack([own] + [moved[s] for s in range(1, N_REP)])
    swapped = swap_tp(mine)
    return jnp.concatenate([mine, swapped], axis=0)


def products(block, normed_ref, u_ref, gg_ref, gu_ref, hid_ref, extra_ref, write):
    contract = (((0,), (0,)), ((), ()))
    for i, (left, right) in enumerate(((normed_ref, gg_ref), (normed_ref, gu_ref), (u_ref, hid_ref))):
        product = lax.dot_general(left[...], right[...], contract, preferred_element_type=F32)
        if i == 0:
            write(0, block - 128, product[:, : block - 128])
            write(block - 128, block, product[:, block - 128 :] + extra_ref[...])
        else:
            write(i * block, (i + 1) * block, product)


def grads_kernel(block, *refs):
    def write(start, stop, value):
        refs[6][:, start:stop] = value.astype(BF16)

    products(block, *refs[:6], write)


def grads_blocks_kernel(rows, block, y_ref, *refs):
    outs, acc = refs[6:10], refs[10]

    def write(start, stop, value):
        acc[:, : stop - start] = value
        for s in range(N_Y):
            first = pl.multiple_of(lax.rem(y_ref[0] + s, N_Y) * rows, rows)
            outs[s][:, start:stop] = acc[pl.ds(first, rows), : stop - start].astype(outs[s].dtype)

    products(block, *refs[:6], write)


def weight_grads(normed, u, gg, gu, hid, extra, y=None):
    tokens, d = normed.shape
    block = gg.shape[1]
    rows = d // N_Y
    if y is None:
        shapes, kernel, scratch, first = [(d, BF16)], functools.partial(grads_kernel, block), [], ()
    else:
        shapes, kernel = [(rows, F32)] + [(rows, BF16)] * 3, functools.partial(grads_blocks_kernel, rows, block)
        scratch, first = [pltpu.VMEM((d, block), F32)], (y.reshape(1),)
    return pl.pallas_call(
        kernel,
        out_shape=[jax.ShapeDtypeStruct((n, 3 * block), dtype) for n, dtype in shapes],
        in_specs=[SMEM] * len(first) + [VMEM] * 6,
        out_specs=[VMEM] * len(shapes),
        scratch_shapes=scratch,
        cost_estimate=pl.CostEstimate(flops=6 * tokens * d * block, bytes_accessed=10000000, transcendentals=0),
        compiler_params=pltpu.CompilerParams(vmem_limit_bytes=48 * 1024 * 1024),
        name="weight_grads",
    )(*first, normed, u, gg, gu, hid, extra)


def narrow(value, lane):
    most = jnp.max(jnp.abs(value), axis=-1, keepdims=True)
    e = jnp.where(most > 0.0, jnp.clip(jnp.ceil(jnp.log2(most)) - 12.0, -120.0, 120.0), 0.0)
    lanes = lax.broadcasted_iota(jnp.int32, value.shape, value.ndim - 1)
    return jnp.where(lanes == lane, e, value * jnp.exp2(-e)).astype(F16)


def widen(value, lane):
    return value.astype(F32) * jnp.exp2(value[..., lane : lane + 1].astype(F32))


def finish_kernel(q, block, layers, r_ref, b0, b1, b2, b3, *refs):
    accums, outs, stack = refs[:3], refs[3:6], refs[6]
    for s, b in enumerate((b0, b1, b2, b3)):
        stack[lax.rem(r_ref[0] + (N_REP - s), N_REP)] = b[...]
    for l in range(layers):
        for i in range(3):
            whole = jnp.concatenate([stack[k, l, :, i * block : i * block + q] for k in range(N_REP)], axis=1)
            outs[i][l] = accums[i][l] + whole


def finish(r, pieces, accums, q, block):
    return pl.pallas_call(
        functools.partial(finish_kernel, q, block, accums[0].shape[0]),
        out_shape=[jax.ShapeDtypeStruct(accums[0].shape, F32)] * 3,
        in_specs=[SMEM] + [VMEM] * 7,
        out_specs=[VMEM] * 3,
        scratch_shapes=[pltpu.VMEM((N_REP,) + pieces[0].shape, F32)],
        cost_estimate=pl.CostEstimate(flops=1000000, bytes_accessed=2000000, transcendentals=0),
        name="finish",
    )(r.reshape(1), *pieces, *accums)


def token_scale(x):
    x = x.astype(F32)
    return lax.rsqrt(jnp.mean(x * x, axis=1, keepdims=True) + epsilon)


def body(
    saved_inputs,
    out_cotangent,
    gate_weight,
    up_weight,
    down_weight,
    norm_gain,
    gate_accum,
    up_accum,
    down_accum,
    gain_accum,
):
    layers, tokens, d = saved_inputs.shape
    rows, hidden_local = gate_weight.shape[1:]
    q = hidden_local // N_REP
    block = -(-(q + 2) // 128) * 128
    half = tokens // 2
    r, f, t = lax.axis_index("rep"), lax.axis_index("fsdp"), lax.axis_index("tp")
    y = f // N_Z

    packed = pack(r, gate_weight, up_weight, down_weight, norm_gain, q, block)
    width = 3 * block
    top, low = layers - 1, 0

    lines = []
    for part in packed[top:]:
        lines.append(exchange(part, "fsdp", Z_GROUPS).reshape(N_Z * rows, part.shape[2]))
    line = lines[-1]
    own_x = lax.dynamic_slice_in_dim(saved_inputs, t * half, half, 1)
    cotangent = lax.dynamic_slice_in_dim(out_cotangent, t * half, half, 0)
    shared = share_tokens(jnp.stack([own_x[top], cotangent.astype(BF16), own_x[low]]), line)
    moved = []
    for part in lines:
        moved.append({s: shift_y(part, s) for s in Y_STEPS})
    x_top = shared[:, 0].reshape(8 * half, d)
    u_top = shared[:, 1].reshape(8 * half, d)
    scale_top = token_scale(x_top)
    moved = after(moved, u_top, scale_top)
    full_top = place(y, *([part] + [m[s] for s in range(1, N_Y)] for part, m in zip(lines, moved))).reshape(d, width)

    low_packed = after(packed[low], line)
    line = exchange(low_packed, "fsdp", Z_GROUPS)
    line_low = line.reshape(N_Z * rows, width)
    cols = (((1,), (1,)), ((), ()))
    pick = (lax.broadcasted_iota(jnp.int32, (8, block), 1) == q).astype(BF16)

    def forward(x, u, w, scale):
        gate_w, up_w, down_w = w[:, :block], w[:, block : 2 * block], w[:, 2 * block :]
        gain = lax.dot_general(pick, gate_w, cols, preferred_element_type=F32)[0]
        white = x.astype(F32) * scale
        normed = (white * gain).astype(BF16)
        gate_pre = jnp.dot(normed, gate_w, preferred_element_type=F32)
        up_pre = jnp.dot(normed, up_w, preferred_element_type=F32)
        sig = jax.nn.sigmoid(gate_pre)
        active = gate_pre * sig
        hidden = (active * up_pre).astype(BF16)
        grad_hidden = jnp.dot(u, down_w, preferred_element_type=F32)
        grad_gate = (grad_hidden * up_pre * (sig * (1.0 + gate_pre * (1.0 - sig)))).astype(BF16)
        grad_up = (grad_hidden * active).astype(BF16)
        return gain, white, normed, hidden, grad_gate, grad_up

    def to_normed(grad_gate, grad_up, w):
        partial = lax.dot_general(grad_gate, w[:, :block], cols, preferred_element_type=F32)
        return partial + lax.dot_general(grad_up, w[:, block : 2 * block], cols, preferred_element_type=F32)

    def gain_columns(partial, white):
        gain_part = jnp.sum(partial * white, axis=0)
        gain_high = gain_part.astype(BF16).astype(F32)
        lane = lax.broadcasted_iota(jnp.int32, (d, 128), 1) - (q - block + 128)
        return jnp.where(lane == 0, gain_high[:, None], jnp.where(lane == 1, (gain_part - gain_high)[:, None], 0.0))

    def step_back(cotangent, own_x, grad_normed, gain):
        own = own_x.astype(F32)
        own_scale = lax.rsqrt(jnp.mean(own * own, axis=1, keepdims=True) + epsilon)
        own_white = own * own_scale
        grad_white = grad_normed * gain
        inner = jnp.mean(grad_white * own_white, axis=1, keepdims=True)
        return cotangent + own_scale * (grad_white - own_white * inner)

    gain, white, normed, hidden, gg, gu = forward(x_top, u_top, full_top, scale_top)
    partial = to_normed(gg, gu, full_top).reshape(8, half, d)
    mine = partial[:4] + swap_tp(partial[4:])
    moved = {s: shift_rep(mine[s], -s) for s in REP_STEPS}
    line_low = after(line_low, mine)
    moved_low = {s: shift_y(line_low, s) for s in (1, 3)}
    moved_low |= {2: shift_y(line_low, 2)}
    extra = gain_columns(partial.reshape(8 * half, d), white)
    (grads_top,) = weight_grads(after(normed, mine), u_top, gg, gu, hidden, extra)
    received = exchange(grads_top.reshape(N_Y, N_Z * rows, width), "fsdp", Y_GROUPS)
    grad_normed = mine[0]
    for s in REP_STEPS:
        grad_normed = grad_normed + moved[s]
    cotangent = step_back(cotangent, own_x[top], grad_normed, gain)

    x_low = shared[:, 2].reshape(8 * half, d)
    u_low = share_tokens(cotangent.astype(BF16)).reshape(8 * half, d)
    moved_low, x_low = after((moved_low, x_low), cotangent, grads_top)
    full_low = place(y, [line_low] + [moved_low[s] for s in range(1, N_Y)]).reshape(d, width)
    gain, white, normed, hidden, gg, gu = forward(x_low, u_low, full_low, token_scale(x_low))
    partial = to_normed(gg, gu, full_low).reshape(8, half, d)
    extra = gain_columns(partial.reshape(8 * half, d), white)
    grads_low = weight_grads(normed, u_low, gg, gu, hidden, extra, y)
    moved_y = {s: shift_y(grads_low[s], s) for s in Y_STEPS}

    partial = after(partial, grads_low)
    mine = partial[:4] + swap_tp(partial[4:])
    moved = {s: shift_rep(mine[s], -s) for s in REP_STEPS}
    grad_normed = mine[0]
    for s in REP_STEPS:
        grad_normed = grad_normed + moved[s]
    cotangent = step_back(cotangent, own_x[low], grad_normed, gain)

    received = after(received, grads_low)
    total = jnp.sum(received.astype(F32), axis=0)
    shard_in = narrow(total, q + 2).reshape(N_Z, rows, width)
    shard_top = exchange(shard_in, "fsdp", Z_GROUPS)
    moved_y = after(moved_y, shard_in, mine)
    total = grads_low[0]
    for s in Y_STEPS:
        total = total + moved_y[s].astype(F32)
    shard_in = narrow(total, q + 2).reshape(N_Z, rows, width)
    shard_low = exchange(shard_in, "fsdp", Z_GROUPS)
    own = jnp.stack([narrow(jnp.sum(widen(v, q + 2), axis=0), q + 2) for v in (shard_low, shard_top)])
    moved = {s: shift_rep(own, s) for s in REP_STEPS}
    pieces = [widen(own, q + 2)] + [widen(moved[s], q + 2) for s in range(1, N_REP)]
    outs = finish(r, pieces, (gate_accum, up_accum, down_accum), q, block)
    gain_sum = sum(jnp.sum(b[:, :, q : q + 2], axis=2) for b in pieces)
    gain_grad = gain_accum + gain_sum + swap_tp(gain_sum)

    other = swap_tp(cotangent)
    both = jnp.stack([cotangent, other])
    cot_out = jnp.concatenate([lax.dynamic_index_in_dim(both, t, 0, False),
                               lax.dynamic_index_in_dim(both, 1 - t, 0, False)], axis=0)
    return (cot_out, outs[0], outs[1], outs[2], gain_grad)


def solution(mesh):
    return jax.shard_map(
        body,
        mesh=mesh,
        in_specs=(
            P(None, ("rep", "fsdp"), None),
            P(("rep", "fsdp"), None),
            P(None, "fsdp", "tp"),
            P(None, "fsdp", "tp"),
            P(None, "fsdp", "tp"),
            P(None, "fsdp"),
            P(None, "fsdp", "tp"),
            P(None, "fsdp", "tp"),
            P(None, "fsdp", "tp"),
            P(None, "fsdp"),
        ),
        out_specs=(
            P(("rep", "fsdp"), None),
            P(None, "fsdp", "tp"),
            P(None, "fsdp", "tp"),
            P(None, "fsdp", "tp"),
            P(None, "fsdp"),
        ),
        check_vma=False,
    )
```

```python
import functools

import jax
import jax.numpy as jnp
from jax import lax
from jax.experimental import pallas as pl
from jax.experimental.pallas import tpu as pltpu
from jax.sharding import PartitionSpec as P

epsilon = 1e-06
F32, BF16, F16 = jnp.float32, jnp.bfloat16, jnp.float16


N_Y, N_Z, N_REP = 4, 8, 4
REP_STEPS = (1, 3, 2)
Y_STEPS = (1, 3, 2)
VMEM = pl.BlockSpec(memory_space=pltpu.VMEM)
SMEM = pl.BlockSpec(memory_space=pltpu.SMEM)


def shift_rep(value, step):
    return lax.ppermute(value, "rep", [(i, (i + step) % N_REP) for i in range(N_REP)])


def swap_tp(value):
    return lax.ppermute(value, "tp", [(0, 1), (1, 0)])


def shift_y(value, step):
    pairs = [(y * N_Z + z, (y + step) % N_Y * N_Z + z) for y in range(N_Y) for z in range(N_Z)]
    return lax.ppermute(value, "fsdp", pairs)


Y_GROUPS = [[y * N_Z + z for y in range(N_Y)] for z in range(N_Z)]
Z_GROUPS = [[y * N_Z + z for z in range(N_Z)] for y in range(N_Y)]


def exchange(value, axis, groups=None):
    return lax.all_to_all(value, axis, 0, 0, tiled=True, axis_index_groups=groups)


def after(value, *others):
    return lax.optimization_barrier((value, others))[0]


def parts_of(width):
    first = -(-width // 256) * 128
    return first, width - first


def pack_kernel(q, block, r_ref, gate_ref, up_ref, down_ref, gain_ref, *refs):
    outs, first, second, one = refs[:-3], *refs[-3:]
    rows = gate_ref.shape[1]
    row = lax.broadcasted_iota(jnp.int32, (rows, rows), 0)
    diagonal = row == lax.broadcasted_iota(jnp.int32, (rows, rows), 1)
    cut = first.shape[-1]
    for l in range(len(outs) + 1):
        gain = jnp.where(diagonal, gain_ref[l : l + 1].astype(F32), 0.0)
        one[...] = jnp.zeros_like(one)
        one[:, q : q + 1] = jnp.sum(gain, axis=1, keepdims=True).astype(BF16)
        for k in range(N_REP):

            @pl.when(r_ref[0] == k)
            def _():
                for i, w in enumerate((gate_ref, up_ref, down_ref)):
                    one[:, i * block : i * block + q] = w[l, :, k * q : (k + 1) * q]

        for i in range(N_Z):
            if l < len(outs):
                outs[l][i] = one[...]
            else:
                first[i] = one[:, :cut]
                second[i] = one[:, cut:]


def pack(r, gate, up, down, gain, q, block):
    layers, rows, _ = gate.shape
    return pl.pallas_call(
        functools.partial(pack_kernel, q, block),
        out_shape=[jax.ShapeDtypeStruct((N_Z, rows, 3 * block), BF16)] * (layers - 1)
        + [jax.ShapeDtypeStruct((N_Z, rows, n), BF16) for n in parts_of(3 * block)],
        in_specs=[SMEM] + [VMEM] * 4,
        out_specs=[VMEM] * (layers + 1),
        scratch_shapes=[pltpu.VMEM((rows, 3 * block), BF16)],
        cost_estimate=pl.CostEstimate(flops=1000000, bytes_accessed=1000000, transcendentals=0),
        name="pack",
    )(r.reshape(1), gate, up, down, gain)


def layer_kernel(parts, q, block, step, y_ref, *refs):
    pieces, (x_ref, u_ref, scale_ref) = refs[: N_Y * parts], refs[N_Y * parts : N_Y * parts + 3]
    normed_ref, gg_ref, gu_ref, hid_ref, mine_ref, other_ref, sum_ref, gain_ref, w = refs[N_Y * parts + 3 :]
    rows = pieces[0].shape[0]
    for s in range(N_Y):
        first = pl.multiple_of(lax.rem(y_ref[0] + (N_Y - s), N_Y) * rows, rows)
        start = 0
        for p in range(parts):
            piece = pieces[p * N_Y + s]
            w[pl.ds(first, rows), start : start + piece.shape[1]] = piece[...]
            start += piece.shape[1]
    gate_w, up_w, down_w = w[:, :block], w[:, block : 2 * block], w[:, 2 * block :]
    cols = (((1,), (1,)), ((), ()))
    pick = (lax.broadcasted_iota(jnp.int32, (8, block), 1) == q).astype(BF16)
    gain = lax.dot_general(pick, gate_w, cols, preferred_element_type=F32)[0:1]
    gain_ref[...] = gain
    tokens = x_ref.shape[0]
    total = jnp.zeros((1, x_ref.shape[1]), F32)
    for start in range(0, tokens, step):
        own = slice(start, start + step)
        white = x_ref[own, :].astype(F32) * scale_ref[own, :]
        normed = (white * gain).astype(BF16)
        normed_ref[own, :] = normed
        gate_pre = jnp.dot(normed, gate_w, preferred_element_type=F32)
        up_pre = jnp.dot(normed, up_w, preferred_element_type=F32)
        grad_hidden = jnp.dot(u_ref[own, :], down_w, preferred_element_type=F32)
        sig = jax.nn.sigmoid(gate_pre)
        active = gate_pre * sig
        hid_ref[own, :] = (active * up_pre).astype(BF16)
        gg = (grad_hidden * up_pre * (sig * (1.0 + gate_pre * (1.0 - sig)))).astype(BF16)
        gu = (grad_hidden * active).astype(BF16)
        gg_ref[own, :] = gg
        gu_ref[own, :] = gu
        partial = lax.dot_general(gg, gate_w, cols, preferred_element_type=F32)
        partial = partial + lax.dot_general(gu, up_w, cols, preferred_element_type=F32)
        total = total + jnp.sum(partial * white, axis=0, keepdims=True)
        if start < tokens // 2:
            mine_ref[own, :] = partial
        else:
            other_ref[start - tokens // 2 : start - tokens // 2 + step, :] = partial
    sum_ref[...] = total


def layer(y, parts, x, u, scale, q, block):
    tokens, d = x.shape
    pieces = [piece for part in parts for piece in part]

    def shape(*dims, dtype=BF16):
        return jax.ShapeDtypeStruct(dims, dtype)

    wide, half = shape(tokens, block), shape(tokens // 2, d, dtype=F32)
    row = shape(1, d, dtype=F32)
    return pl.pallas_call(
        functools.partial(layer_kernel, len(parts), q, block, 256),
        out_shape=[shape(tokens, d), wide, wide, wide, half, half, row, row],
        in_specs=[SMEM] + [VMEM] * (len(pieces) + 3),
        out_specs=[VMEM] * 8,
        scratch_shapes=[pltpu.VMEM((d, 3 * block), BF16)],
        cost_estimate=pl.CostEstimate(flops=10 * tokens * d * block, bytes_accessed=15000000, transcendentals=tokens * block),
        compiler_params=pltpu.CompilerParams(vmem_limit_bytes=56 * 1024 * 1024),
        name="layer",
    )(y.reshape(1), *pieces, x, u, scale)


def share_tokens(own, *others):
    moved = {s: shift_rep(own, s) for s in REP_STEPS}
    if others:
        moved = after(moved, *others)
    mine = jnp.stack([own] + [moved[s] for s in range(1, N_REP)])
    swapped = swap_tp(mine)
    return jnp.concatenate([mine, swapped], axis=0)


def products(block, normed_ref, u_ref, gg_ref, gu_ref, hid_ref, extra_ref, write):
    contract = (((0,), (0,)), ((), ()))
    for i, (left, right) in enumerate(((normed_ref, gg_ref), (normed_ref, gu_ref), (u_ref, hid_ref))):
        product = lax.dot_general(left[...], right[...], contract, preferred_element_type=F32)
        if i == 0:
            write(0, block - 128, product[:, : block - 128])
            write(block - 128, block, product[:, block - 128 :] + extra_ref[...])
        else:
            write(i * block, (i + 1) * block, product)


def grads_kernel(block, *refs):
    def write(start, stop, value):
        refs[6][:, start:stop] = value.astype(BF16)

    products(block, *refs[:6], write)


def grads_blocks_kernel(rows, block, y_ref, *refs):
    outs, acc = refs[6:10], refs[10]

    def write(start, stop, value):
        acc[:, : stop - start] = value
        for s in range(N_Y):
            first = pl.multiple_of(lax.rem(y_ref[0] + s, N_Y) * rows, rows)
            outs[s][:, start:stop] = acc[pl.ds(first, rows), : stop - start].astype(outs[s].dtype)

    products(block, *refs[:6], write)


def weight_grads(normed, u, gg, gu, hid, extra, y=None):
    tokens, d = normed.shape
    block = gg.shape[1]
    rows = d // N_Y
    if y is None:
        shapes, kernel, scratch, first = [(d, BF16)], functools.partial(grads_kernel, block), [], ()
    else:
        shapes, kernel = [(rows, F32)] + [(rows, BF16)] * 3, functools.partial(grads_blocks_kernel, rows, block)
        scratch, first = [pltpu.VMEM((d, block), F32)], (y.reshape(1),)
    return pl.pallas_call(
        kernel,
        out_shape=[jax.ShapeDtypeStruct((n, 3 * block), dtype) for n, dtype in shapes],
        in_specs=[SMEM] * len(first) + [VMEM] * 6,
        out_specs=[VMEM] * len(shapes),
        scratch_shapes=scratch,
        cost_estimate=pl.CostEstimate(flops=6 * tokens * d * block, bytes_accessed=10000000, transcendentals=0),
        compiler_params=pltpu.CompilerParams(vmem_limit_bytes=48 * 1024 * 1024),
        name="weight_grads",
    )(*first, normed, u, gg, gu, hid, extra)


def narrow(value, lane):
    most = jnp.max(jnp.abs(value), axis=-1, keepdims=True)
    e = jnp.where(most > 0.0, jnp.clip(jnp.ceil(jnp.log2(most)) - 12.0, -120.0, 120.0), 0.0)
    lanes = lax.broadcasted_iota(jnp.int32, value.shape, value.ndim - 1)
    return jnp.where(lanes == lane, e, value * jnp.exp2(-e)).astype(F16)


def widen(value, lane):
    return value.astype(F32) * jnp.exp2(value[..., lane : lane + 1].astype(F32))


def finish_kernel(q, block, layers, r_ref, b0, b1, b2, b3, *refs):
    accums, outs, stack = refs[:3], refs[3:6], refs[6]
    for s, b in enumerate((b0, b1, b2, b3)):
        stack[lax.rem(r_ref[0] + (N_REP - s), N_REP)] = b[...]
    for l in range(layers):
        for i in range(3):
            whole = jnp.concatenate([stack[k, l, :, i * block : i * block + q] for k in range(N_REP)], axis=1)
            outs[i][l] = accums[i][l] + whole


def finish(r, pieces, accums, q, block):
    return pl.pallas_call(
        functools.partial(finish_kernel, q, block, accums[0].shape[0]),
        out_shape=[jax.ShapeDtypeStruct(accums[0].shape, F32)] * 3,
        in_specs=[SMEM] + [VMEM] * 7,
        out_specs=[VMEM] * 3,
        scratch_shapes=[pltpu.VMEM((N_REP,) + pieces[0].shape, F32)],
        cost_estimate=pl.CostEstimate(flops=1000000, bytes_accessed=2000000, transcendentals=0),
        name="finish",
    )(r.reshape(1), *pieces, *accums)


def token_scale(x):
    x = x.astype(F32)
    return lax.rsqrt(jnp.mean(x * x, axis=1, keepdims=True) + epsilon)


def body(
    saved_inputs,
    out_cotangent,
    gate_weight,
    up_weight,
    down_weight,
    norm_gain,
    gate_accum,
    up_accum,
    down_accum,
    gain_accum,
):
    layers, tokens, d = saved_inputs.shape
    rows, hidden_local = gate_weight.shape[1:]
    q = hidden_local // N_REP
    block = -(-(q + 2) // 128) * 128
    half = tokens // 2
    r, f, t = lax.axis_index("rep"), lax.axis_index("fsdp"), lax.axis_index("tp")
    y = f // N_Z

    packed = pack(r, gate_weight, up_weight, down_weight, norm_gain, q, block)
    width = 3 * block
    top, low = layers - 1, 0

    lines = []
    for part in packed[top:]:
        lines.append(exchange(part, "fsdp", Z_GROUPS).reshape(N_Z * rows, part.shape[2]))
    line = lines[-1]
    own_x = lax.dynamic_slice_in_dim(saved_inputs, t * half, half, 1)
    cotangent = lax.dynamic_slice_in_dim(out_cotangent, t * half, half, 0)
    shared = share_tokens(jnp.stack([own_x[top], cotangent.astype(BF16), own_x[low]]), line)
    moved = []
    for part in lines:
        moved.append({s: shift_y(part, s) for s in Y_STEPS})
    x_top = shared[:, 0].reshape(8 * half, d)
    u_top = shared[:, 1].reshape(8 * half, d)
    scale_top = token_scale(x_top)
    moved = after(moved, u_top, scale_top)
    weights_top = [[part] + [m[s] for s in range(1, N_Y)] for part, m in zip(lines, moved)]

    low_packed = after(packed[low], line)
    line = exchange(low_packed, "fsdp", Z_GROUPS)
    line_low = line.reshape(N_Z * rows, width)

    def gain_columns(total):
        gain_part = total[0]
        gain_high = gain_part.astype(BF16).astype(F32)
        lane = lax.broadcasted_iota(jnp.int32, (d, 128), 1) - (q - block + 128)
        return jnp.where(lane == 0, gain_high[:, None], jnp.where(lane == 1, (gain_part - gain_high)[:, None], 0.0))

    def step_back(cotangent, own_x, grad_normed, gain):
        own = own_x.astype(F32)
        own_scale = lax.rsqrt(jnp.mean(own * own, axis=1, keepdims=True) + epsilon)
        own_white = own * own_scale
        grad_white = grad_normed * gain
        inner = jnp.mean(grad_white * own_white, axis=1, keepdims=True)
        return cotangent + own_scale * (grad_white - own_white * inner)

    normed, gg, gu, hidden, mine, other, total, gain = layer(y, weights_top, x_top, u_top, scale_top, q, block)
    mine = (mine + swap_tp(other)).reshape(4, half, d)
    moved = {s: shift_rep(mine[s], -s) for s in REP_STEPS}
    line_low = after(line_low, mine)
    moved_low = {2: shift_y(line_low, 2)}
    moved_low |= {s: shift_y(line_low, s) for s in (1, 3)}
    extra = gain_columns(total)
    (grads_top,) = weight_grads(after(normed, mine), u_top, gg, gu, hidden, extra)
    received = exchange(grads_top.reshape(N_Y, N_Z * rows, width), "fsdp", Y_GROUPS)
    grad_normed = mine[0]
    for s in REP_STEPS:
        grad_normed = grad_normed + moved[s]
    cotangent = step_back(cotangent, own_x[top], grad_normed, gain)

    x_low = shared[:, 2].reshape(8 * half, d)
    u_low = share_tokens(cotangent.astype(BF16)).reshape(8 * half, d)
    moved_low, x_low = after((moved_low, x_low), cotangent, grads_top)
    weights_low = [[line_low] + [moved_low[s] for s in range(1, N_Y)]]
    normed, gg, gu, hidden, mine, other, total, gain = layer(y, weights_low, x_low, u_low, token_scale(x_low), q, block)
    extra = gain_columns(total)
    grads_low = weight_grads(normed, u_low, gg, gu, hidden, extra, y)
    moved_y = {s: shift_y(grads_low[s], s) for s in Y_STEPS}

    mine, other = after((mine, other), grads_low)
    mine = (mine + swap_tp(other)).reshape(4, half, d)
    moved = {s: shift_rep(mine[s], -s) for s in REP_STEPS}
    grad_normed = mine[0]
    for s in REP_STEPS:
        grad_normed = grad_normed + moved[s]
    cotangent = step_back(cotangent, own_x[low], grad_normed, gain)

    received = after(received, grads_low)
    total = jnp.sum(received.astype(F32), axis=0)
    shard_in = narrow(total, q + 2).reshape(N_Z, rows, width)
    shard_top = exchange(shard_in, "fsdp", Z_GROUPS)
    moved_y = after(moved_y, shard_in, mine)
    total = grads_low[0]
    for s in Y_STEPS:
        total = total + moved_y[s].astype(F32)
    shard_in = narrow(total, q + 2).reshape(N_Z, rows, width)
    shard_low = exchange(shard_in, "fsdp", Z_GROUPS)
    own = jnp.stack([narrow(jnp.sum(widen(v, q + 2), axis=0), q + 2) for v in (shard_low, shard_top)])
    moved = {s: shift_rep(own, s) for s in REP_STEPS}
    pieces = [widen(own, q + 2)] + [widen(moved[s], q + 2) for s in range(1, N_REP)]
    outs = finish(r, pieces, (gate_accum, up_accum, down_accum), q, block)
    gain_sum = sum(jnp.sum(b[:, :, q : q + 2], axis=2) for b in pieces)
    gain_grad = gain_accum + gain_sum + swap_tp(gain_sum)

    other = swap_tp(cotangent)
    both = jnp.stack([cotangent, other])
    cot_out = jnp.concatenate([lax.dynamic_index_in_dim(both, t, 0, False),
                               lax.dynamic_index_in_dim(both, 1 - t, 0, False)], axis=0)
    return (cot_out, outs[0], outs[1], outs[2], gain_grad)


def solution(mesh):
    return jax.shard_map(
        body,
        mesh=mesh,
        in_specs=(
            P(None, ("rep", "fsdp"), None),
            P(("rep", "fsdp"), None),
            P(None, "fsdp", "tp"),
            P(None, "fsdp", "tp"),
            P(None, "fsdp", "tp"),
            P(None, "fsdp"),
            P(None, "fsdp", "tp"),
            P(None, "fsdp", "tp"),
            P(None, "fsdp", "tp"),
            P(None, "fsdp"),
        ),
        out_specs=(
            P(("rep", "fsdp"), None),
            P(None, "fsdp", "tp"),
            P(None, "fsdp", "tp"),
            P(None, "fsdp", "tp"),
            P(None, "fsdp"),
        ),
        check_vma=False,
    )
```

```python
import functools

import jax
import jax.numpy as jnp
from jax import lax
from jax.experimental import pallas as pl
from jax.experimental.pallas import tpu as pltpu
from jax.sharding import PartitionSpec as P

epsilon = 1e-06
F32, BF16, F16 = jnp.float32, jnp.bfloat16, jnp.float16


N_Y, N_Z, N_REP = 4, 8, 4
REP_STEPS = (1, 3, 2)
Y_STEPS = (1, 3, 2)
VMEM = pl.BlockSpec(memory_space=pltpu.VMEM)
SMEM = pl.BlockSpec(memory_space=pltpu.SMEM)


def shift_rep(value, step):
    return lax.ppermute(value, "rep", [(i, (i + step) % N_REP) for i in range(N_REP)])


def swap_tp(value):
    return lax.ppermute(value, "tp", [(0, 1), (1, 0)])


def shift_y(value, step):
    pairs = [(y * N_Z + z, (y + step) % N_Y * N_Z + z) for y in range(N_Y) for z in range(N_Z)]
    return lax.ppermute(value, "fsdp", pairs)


Y_GROUPS = [[y * N_Z + z for y in range(N_Y)] for z in range(N_Z)]
Z_GROUPS = [[y * N_Z + z for z in range(N_Z)] for y in range(N_Y)]


def exchange(value, axis, groups=None):
    return lax.all_to_all(value, axis, 0, 0, tiled=True, axis_index_groups=groups)


def after(value, *others):
    return lax.optimization_barrier((value, others))[0]


def parts_of(width):
    first = -(-width // 256) * 128
    return first, width - first


def pack_kernel(q, block, r_ref, gate_ref, up_ref, down_ref, gain_ref, *refs):
    outs, first, second, one = refs[:-3], *refs[-3:]
    rows = gate_ref.shape[1]
    row = lax.broadcasted_iota(jnp.int32, (rows, rows), 0)
    diagonal = row == lax.broadcasted_iota(jnp.int32, (rows, rows), 1)
    cut = first.shape[-1]
    for l in range(len(outs) + 1):
        gain = jnp.where(diagonal, gain_ref[l : l + 1].astype(F32), 0.0)
        one[...] = jnp.zeros_like(one)
        one[:, q : q + 1] = jnp.sum(gain, axis=1, keepdims=True).astype(BF16)
        for k in range(N_REP):

            @pl.when(r_ref[0] == k)
            def _():
                for i, w in enumerate((gate_ref, up_ref, down_ref)):
                    one[:, i * block : i * block + q] = w[l, :, k * q : (k + 1) * q]

        for i in range(N_Z):
            if l < len(outs):
                outs[l][i] = one[...]
            else:
                first[i] = one[:, :cut]
                second[i] = one[:, cut:]


def pack(r, gate, up, down, gain, q, block):
    layers, rows, _ = gate.shape
    return pl.pallas_call(
        functools.partial(pack_kernel, q, block),
        out_shape=[jax.ShapeDtypeStruct((N_Z, rows, 3 * block), BF16)] * (layers - 1)
        + [jax.ShapeDtypeStruct((N_Z, rows, n), BF16) for n in parts_of(3 * block)],
        in_specs=[SMEM] + [VMEM] * 4,
        out_specs=[VMEM] * (layers + 1),
        scratch_shapes=[pltpu.VMEM((rows, 3 * block), BF16)],
        cost_estimate=pl.CostEstimate(flops=1000000, bytes_accessed=1000000, transcendentals=0),
        name="pack",
    )(r.reshape(1), gate, up, down, gain)


def layer_kernel(parts, q, block, step, grads, y_ref, *refs):
    pieces, (x_ref, u_ref) = refs[: N_Y * parts], refs[N_Y * parts : N_Y * parts + 2]
    mine_ref, other_ref, gain_ref = refs[N_Y * parts + 2 : N_Y * parts + 5]
    if grads:
        *blocks, normed_ref, gg_ref, gu_ref, hid_ref, w, acc = refs[N_Y * parts + 5 :]
    else:
        sum_ref, normed_ref, gg_ref, gu_ref, hid_ref, w = refs[N_Y * parts + 5 :]
    rows = pieces[0].shape[0]
    for s in range(N_Y):
        first = pl.multiple_of(lax.rem(y_ref[0] + (N_Y - s), N_Y) * rows, rows)
        start = 0
        for p in range(parts):
            piece = pieces[p * N_Y + s]
            w[pl.ds(first, rows), start : start + piece.shape[1]] = piece[...]
            start += piece.shape[1]
    gate_w, up_w, down_w = w[:, :block], w[:, block : 2 * block], w[:, 2 * block :]
    cols = (((1,), (1,)), ((), ()))
    pick = (lax.broadcasted_iota(jnp.int32, (8, block), 1) == q).astype(BF16)
    gain = lax.dot_general(pick, gate_w, cols, preferred_element_type=F32)[0:1]
    gain_ref[...] = gain
    tokens = x_ref.shape[0]
    total = jnp.zeros((1, x_ref.shape[1]), F32)
    for start in range(0, tokens, step):
        own = slice(start, start + step)
        x = x_ref[own, :].astype(F32)
        white = x * lax.rsqrt(jnp.mean(x * x, axis=1, keepdims=True) + epsilon)
        normed = (white * gain).astype(BF16)
        normed_ref[own, :] = normed
        gate_pre = jnp.dot(normed, gate_w, preferred_element_type=F32)
        up_pre = jnp.dot(normed, up_w, preferred_element_type=F32)
        grad_hidden = jnp.dot(u_ref[own, :], down_w, preferred_element_type=F32)
        sig = jax.nn.sigmoid(gate_pre)
        active = gate_pre * sig
        hid_ref[own, :] = (active * up_pre).astype(BF16)
        gg = (grad_hidden * up_pre * (sig * (1.0 + gate_pre * (1.0 - sig)))).astype(BF16)
        gu = (grad_hidden * active).astype(BF16)
        gg_ref[own, :] = gg
        gu_ref[own, :] = gu
        partial = lax.dot_general(gg, gate_w, cols, preferred_element_type=F32)
        partial = partial + lax.dot_general(gu, up_w, cols, preferred_element_type=F32)
        total = total + jnp.sum(partial * white, axis=0, keepdims=True)
        if start < tokens // 2:
            mine_ref[own, :] = partial
        else:
            other_ref[start - tokens // 2 : start - tokens // 2 + step, :] = partial
    if not grads:
        sum_ref[...] = total
        return
    column = jnp.broadcast_to(total, (8, total.shape[1])).T[:, 0:1]
    high = column.astype(BF16).astype(F32)
    contract = (((0,), (0,)), ((), ()))
    for i, (left, right) in enumerate(((normed_ref, gg_ref), (normed_ref, gu_ref), (u_ref, hid_ref))):
        acc[...] = lax.dot_general(left[...], right[...], contract, preferred_element_type=F32)
        if i == 0:
            acc[:, q : q + 1] = high
            acc[:, q + 1 : q + 2] = column - high
        for s in range(N_Y):
            first = pl.multiple_of(lax.rem(y_ref[0] + s, N_Y) * rows, rows)
            blocks[s][:, i * block : (i + 1) * block] = acc[pl.ds(first, rows), :].astype(blocks[s].dtype)


def layer(y, parts, x, u, q, block, grads):
    tokens, d = x.shape
    pieces = [piece for part in parts for piece in part]
    kept = [((tokens, d), BF16)] + [((tokens, block), BF16)] * 3
    outs = [((tokens // 2, d), F32)] * 2 + [((1, d), F32)]
    scratch = [pltpu.VMEM((d, 3 * block), BF16)]
    if grads:
        outs += [((d // N_Y, 3 * block), F32 if s == 0 else BF16) for s in range(N_Y)]
        scratch = [pltpu.VMEM(*k) for k in kept] + scratch + [pltpu.VMEM((d, block), F32)]
    else:
        outs += [((1, d), F32)] + kept
    return pl.pallas_call(
        functools.partial(layer_kernel, len(parts), q, block, 256, grads),
        out_shape=[jax.ShapeDtypeStruct(*o) for o in outs],
        in_specs=[SMEM] + [VMEM] * (len(pieces) + 2),
        out_specs=[VMEM] * len(outs),
        scratch_shapes=scratch,
        cost_estimate=pl.CostEstimate(flops=(16 if grads else 10) * tokens * d * block, bytes_accessed=15000000,
                                      transcendentals=tokens * block),
        compiler_params=pltpu.CompilerParams(vmem_limit_bytes=56 * 1024 * 1024),
        name="layer",
    )(y.reshape(1), *pieces, x, u)


def share_tokens(own, *others):
    moved = {s: shift_rep(own, s) for s in REP_STEPS}
    if others:
        moved = after(moved, *others)
    mine = jnp.stack([own] + [moved[s] for s in range(1, N_REP)])
    swapped = swap_tp(mine)
    return jnp.concatenate([mine, swapped], axis=0)


def products(block, normed_ref, u_ref, gg_ref, gu_ref, hid_ref, extra_ref, write):
    contract = (((0,), (0,)), ((), ()))
    for i, (left, right) in enumerate(((normed_ref, gg_ref), (normed_ref, gu_ref), (u_ref, hid_ref))):
        product = lax.dot_general(left[...], right[...], contract, preferred_element_type=F32)
        if i == 0:
            write(0, block - 128, product[:, : block - 128])
            write(block - 128, block, product[:, block - 128 :] + extra_ref[...])
        else:
            write(i * block, (i + 1) * block, product)


def grads_kernel(block, *refs):
    def write(start, stop, value):
        refs[6][:, start:stop] = value.astype(BF16)

    products(block, *refs[:6], write)


def weight_grads(normed, u, gg, gu, hid, extra):
    tokens, d = normed.shape
    block = gg.shape[1]
    return pl.pallas_call(
        functools.partial(grads_kernel, block),
        out_shape=jax.ShapeDtypeStruct((d, 3 * block), BF16),
        in_specs=[VMEM] * 6,
        out_specs=VMEM,
        cost_estimate=pl.CostEstimate(flops=6 * tokens * d * block, bytes_accessed=10000000, transcendentals=0),
        compiler_params=pltpu.CompilerParams(vmem_limit_bytes=48 * 1024 * 1024),
        name="weight_grads",
    )(normed, u, gg, gu, hid, extra)


def narrow(value, lane):
    most = jnp.max(jnp.abs(value), axis=-1, keepdims=True)
    e = jnp.where(most > 0.0, jnp.clip(jnp.ceil(jnp.log2(most)) - 12.0, -120.0, 120.0), 0.0)
    lanes = lax.broadcasted_iota(jnp.int32, value.shape, value.ndim - 1)
    return jnp.where(lanes == lane, e, value * jnp.exp2(-e)).astype(F16)


def widen(value, lane):
    return value.astype(F32) * jnp.exp2(value[..., lane : lane + 1].astype(F32))


def finish_kernel(q, block, layers, r_ref, b0, b1, b2, b3, *refs):
    accums, outs, stack = refs[:3], refs[3:6], refs[6]
    for s, b in enumerate((b0, b1, b2, b3)):
        stack[lax.rem(r_ref[0] + (N_REP - s), N_REP)] = b[...]
    for l in range(layers):
        for i in range(3):
            whole = jnp.concatenate([stack[k, l, :, i * block : i * block + q] for k in range(N_REP)], axis=1)
            outs[i][l] = accums[i][l] + whole


def finish(r, pieces, accums, q, block):
    return pl.pallas_call(
        functools.partial(finish_kernel, q, block, accums[0].shape[0]),
        out_shape=[jax.ShapeDtypeStruct(accums[0].shape, F32)] * 3,
        in_specs=[SMEM] + [VMEM] * 7,
        out_specs=[VMEM] * 3,
        scratch_shapes=[pltpu.VMEM((N_REP,) + pieces[0].shape, F32)],
        cost_estimate=pl.CostEstimate(flops=1000000, bytes_accessed=2000000, transcendentals=0),
        name="finish",
    )(r.reshape(1), *pieces, *accums)


def body(
    saved_inputs,
    out_cotangent,
    gate_weight,
    up_weight,
    down_weight,
    norm_gain,
    gate_accum,
    up_accum,
    down_accum,
    gain_accum,
):
    layers, tokens, d = saved_inputs.shape
    rows, hidden_local = gate_weight.shape[1:]
    q = hidden_local // N_REP
    block = -(-(q + 2) // 128) * 128
    half = tokens // 2
    r, f, t = lax.axis_index("rep"), lax.axis_index("fsdp"), lax.axis_index("tp")
    y = f // N_Z

    packed = pack(r, gate_weight, up_weight, down_weight, norm_gain, q, block)
    width = 3 * block
    top, low = layers - 1, 0

    lines = []
    for part in packed[top:]:
        lines.append(exchange(part, "fsdp", Z_GROUPS).reshape(N_Z * rows, part.shape[2]))
    line = lines[-1]
    own_x = lax.dynamic_slice_in_dim(saved_inputs, t * half, half, 1)
    cotangent = lax.dynamic_slice_in_dim(out_cotangent, t * half, half, 0)
    shared = share_tokens(jnp.stack([own_x[top], cotangent.astype(BF16), own_x[low]]), line)
    moved = []
    for part in lines:
        moved.append({s: shift_y(part, s) for s in Y_STEPS})
    x_top = shared[:, 0].reshape(8 * half, d)
    u_top = shared[:, 1].reshape(8 * half, d)
    moved = after(moved, u_top, x_top)
    weights_top = [[part] + [m[s] for s in range(1, N_Y)] for part, m in zip(lines, moved)]

    low_packed = after(packed[low], line)
    line = exchange(low_packed, "fsdp", Z_GROUPS)
    line_low = line.reshape(N_Z * rows, width)

    def gain_columns(total):
        gain_part = total[0]
        gain_high = gain_part.astype(BF16).astype(F32)
        lane = lax.broadcasted_iota(jnp.int32, (d, 128), 1) - (q - block + 128)
        return jnp.where(lane == 0, gain_high[:, None], jnp.where(lane == 1, (gain_part - gain_high)[:, None], 0.0))

    def step_back(cotangent, own_x, grad_normed, gain):
        own = own_x.astype(F32)
        own_scale = lax.rsqrt(jnp.mean(own * own, axis=1, keepdims=True) + epsilon)
        own_white = own * own_scale
        grad_white = grad_normed * gain
        inner = jnp.mean(grad_white * own_white, axis=1, keepdims=True)
        return cotangent + own_scale * (grad_white - own_white * inner)

    mine, other, gain, total, normed, gg, gu, hidden = layer(y, weights_top, x_top, u_top, q, block, False)
    mine = (mine + swap_tp(other)).reshape(4, half, d)
    moved = {s: shift_rep(mine[s], -s) for s in REP_STEPS}
    line_low = after(line_low, mine)
    moved_low = {2: shift_y(line_low, 2)}
    moved_low |= {s: shift_y(line_low, s) for s in (1, 3)}
    extra = gain_columns(total)
    grads_top = weight_grads(after(normed, mine), u_top, gg, gu, hidden, extra)
    received = exchange(grads_top.reshape(N_Y, N_Z * rows, width), "fsdp", Y_GROUPS)
    grad_normed = mine[0]
    for s in REP_STEPS:
        grad_normed = grad_normed + moved[s]
    cotangent = step_back(cotangent, own_x[top], grad_normed, gain)

    x_low = shared[:, 2].reshape(8 * half, d)
    u_low = share_tokens(cotangent.astype(BF16)).reshape(8 * half, d)
    moved_low, x_low = after((moved_low, x_low), cotangent, grads_top)
    weights_low = [[line_low] + [moved_low[s] for s in range(1, N_Y)]]
    mine, other, gain, *grads_low = layer(y, weights_low, x_low, u_low, q, block, True)
    moved_y = {s: shift_y(grads_low[s], s) for s in Y_STEPS}

    mine, other = after((mine, other), grads_low)
    mine = (mine + swap_tp(other)).reshape(4, half, d)
    moved = {s: shift_rep(mine[s], -s) for s in REP_STEPS}
    grad_normed = mine[0]
    for s in REP_STEPS:
        grad_normed = grad_normed + moved[s]
    cotangent = step_back(cotangent, own_x[low], grad_normed, gain)

    received = after(received, grads_low)
    total = jnp.sum(received.astype(F32), axis=0)
    shard_in = narrow(total, q + 2).reshape(N_Z, rows, width)
    shard_top = exchange(shard_in, "fsdp", Z_GROUPS)
    moved_y = after(moved_y, shard_in, mine)
    total = grads_low[0]
    for s in Y_STEPS:
        total = total + moved_y[s].astype(F32)
    shard_in = narrow(total, q + 2).reshape(N_Z, rows, width)
    shard_low = exchange(shard_in, "fsdp", Z_GROUPS)
    own = jnp.stack([narrow(jnp.sum(widen(v, q + 2), axis=0), q + 2) for v in (shard_low, shard_top)])
    moved = {s: shift_rep(own, s) for s in REP_STEPS}
    pieces = [widen(own, q + 2)] + [widen(moved[s], q + 2) for s in range(1, N_REP)]
    outs = finish(r, pieces, (gate_accum, up_accum, down_accum), q, block)
    gain_sum = sum(jnp.sum(b[:, :, q : q + 2], axis=2) for b in pieces)
    gain_grad = gain_accum + gain_sum + swap_tp(gain_sum)

    other = swap_tp(cotangent)
    both = jnp.stack([cotangent, other])
    cot_out = jnp.concatenate([lax.dynamic_index_in_dim(both, t, 0, False),
                               lax.dynamic_index_in_dim(both, 1 - t, 0, False)], axis=0)
    return (cot_out, outs[0], outs[1], outs[2], gain_grad)


def solution(mesh):
    return jax.shard_map(
        body,
        mesh=mesh,
        in_specs=(
            P(None, ("rep", "fsdp"), None),
            P(("rep", "fsdp"), None),
            P(None, "fsdp", "tp"),
            P(None, "fsdp", "tp"),
            P(None, "fsdp", "tp"),
            P(None, "fsdp"),
            P(None, "fsdp", "tp"),
            P(None, "fsdp", "tp"),
            P(None, "fsdp", "tp"),
            P(None, "fsdp"),
        ),
        out_specs=(
            P(("rep", "fsdp"), None),
            P(None, "fsdp", "tp"),
            P(None, "fsdp", "tp"),
            P(None, "fsdp", "tp"),
            P(None, "fsdp"),
        ),
        check_vma=False,
    )
```
